1024 devices in a mesh: band: 64 (over z_lo, y), mem: 16 (over z_hi, x, core).
Axes of the slice: x: 4, y: 4, z: 32 (z_hi: 2, z_lo: 16; z = z_hi * 16 + z_lo), core: 2. Of those that a mesh axis runs over, the one named last changes fastest.
Arguments:
- ensemble: float32 [128, 5, 256, 128], P('mem', None, 'band'), may hold values from -5 to 5
- obs_value: float32 [2048, 128], P(('band', 'mem')), may hold values from -6 to 6
- obs_site: int32 [2048, 128], P(('band', 'mem')), may hold values from 0 to 79
- obs_count: int32 [2048], P(('band', 'mem')), may hold values from 32 to 128
- obs_precision: float32 [2048, 128], P(('band', 'mem')), may hold values from 0.25 to 4
- loc_weight: float32 [2048, 3], P(('band', 'mem')), may hold values from 0.1 to 1
- neighbours: int32 [2048, 3], P(('band', 'mem')), may hold values from 0 to 1
Outputs:
- forecast: float32 [128, 5, 256, 128], P('mem', None, 'band')
The draws below stay inside these ranges and needn't reach their ends.
Inputs may be any that keep to these rules, and one draw needn't show every extreme that they name: `obs_site`: site v * 16 + c observes variable v at the tile's c-th cell. Slots 0 to obs_count - 1 of a tile are live. `neighbours`: entries are positions within the aligned block of 2 tiles that holds the tile.
All inputs are finite; a program needn't handle non-finite values.
Results may differ from the reference program's by a relative error of at most 0.0003.
Values sent between devices are 32-bit elements; how exact they have to be, the bound alone decides.
No kernel may reach another device: no remote copies, remote signals or barrier semaphores. Data moves between devices by JAX's collectives and lax.ppermute only.
A program may use at most 32 MiB of HBM per device.

```python
import math
import jax
import jax.numpy as jnp
from jax import lax

M = 128
V = 5
NLON = 128
TILE = 16
OBS = 128
NB = 3
NSI = 6
STEPS = 2
NLAT = 256
TILES = 2048
TILES_A = 2


def set_ends(result, rng, least, high):
    spot = [jax.random.randint(jax.random.fold_in(rng, axis), (), 0, length) for axis, length in enumerate(result.shape)]
    main_axis = result.shape.index(max(result.shape))
    beside = spot[:main_axis] + [(spot[main_axis] + 1) % result.shape[main_axis]] + spot[main_axis + 1:]
    return result.at[tuple(spot)].set(least).at[tuple(beside)].set(high)


def block_scale(key, shape, shards, smallest, top_value):
    def one(position, blocks):
        draws = jax.random.uniform(jax.random.fold_in(jax.random.fold_in(key, 6), position), (blocks,), jnp.float32, smallest / len(shards), top_value / len(shards))
        return jnp.repeat(jnp.exp(draws), shape[position] // blocks).reshape((-1,) + (1,) * (len(shape) - position - 1))

    loudness = one(*shards[0])
    for cut in shards[1:]:
        loudness = loudness * one(*cut)
    return loudness


def normal_values(own_key, shape, width, limit, shards=(), held_as=jnp.bfloat16):
    level = block_scale(own_key, shape, shards, -0.22, 0.18) if shards else 1.0
    entries = jax.random.normal(own_key, shape, jnp.float32) * width * level
    return jnp.minimum(jnp.maximum(entries, -limit), limit).astype(held_as)


def setup_inputs(seed: int = 0) -> dict:
    streams_of = jax.random.split(jax.random.key(seed), 8)
    return {
        "ensemble": normal_values(streams_of[0], (M, V, NLAT, NLON), 1.0, 5.0, ((0, 16), (2, 64)), jnp.float32),
        "obs_value": normal_values(streams_of[1], (TILES, OBS), 1.5, 6.0, ((0, 1024),), jnp.float32),
        "obs_site": set_ends(jax.random.randint(streams_of[2], (TILES, OBS), 0, V * TILE), jax.random.fold_in(streams_of[2], 1), 0, (V * TILE) - 1).astype(jnp.int32),
        "obs_count": set_ends(jax.random.randint(streams_of[3], (TILES,), OBS // 4, OBS + 1), jax.random.fold_in(streams_of[3], 1), OBS // 4, OBS).astype(jnp.int32),
        "obs_precision": jnp.clip(jnp.exp(math.log(4.0) - 2.7725887 * jax.random.uniform(streams_of[4], (TILES, OBS), jnp.float32) ** block_scale(streams_of[4], (TILES, OBS), ((0, 1024),), -0.2, 0.2)), 0.25, 4.0),
        "loc_weight": jnp.clip(jnp.exp(math.log(1.0) - 2.3025851 * jax.random.uniform(streams_of[5], (TILES, NB), jnp.float32) ** block_scale(streams_of[5], (TILES, NB), ((0, 1024),), -0.2, 0.2)), 0.1, 1.0),
        "neighbours": set_ends(jax.random.randint(streams_of[6], (TILES, NB), 0, TILES_A), jax.random.fold_in(streams_of[6], 1), 0, TILES_A - 1).astype(jnp.int32),
    }


COURANT = 0.08
HIGHEST = lax.Precision.HIGHEST

def minmod(lower_jump, upper_jump):
    return jnp.maximum(0.0, jnp.minimum(lower_jump, upper_jump)) + jnp.minimum(0.0, jnp.maximum(lower_jump, upper_jump))

def flux_divergence(halo_extended_field, sweep_direction, advected_field):
    extent = halo_extended_field.shape[sweep_direction]
    differences = lax.slice_in_dim(halo_extended_field, 1, extent, axis=sweep_direction) - lax.slice_in_dim(halo_extended_field, 0, extent - 1, axis=sweep_direction)
    slopes = minmod(lax.slice_in_dim(differences, 0, extent - 2, axis=sweep_direction), lax.slice_in_dim(differences, 1, extent - 1, axis=sweep_direction))
    state_left_side = lax.slice_in_dim(halo_extended_field, 1, extent - 2, axis=sweep_direction) + 0.5 * lax.slice_in_dim(slopes, 0, extent - 3, axis=sweep_direction)
    state_right_side = lax.slice_in_dim(halo_extended_field, 2, extent - 1, axis=sweep_direction) - 0.5 * lax.slice_in_dim(slopes, 1, extent - 2, axis=sweep_direction)
    advected_field_left = state_left_side[:, advected_field:advected_field + 1]
    advected_field_right = state_right_side[:, advected_field:advected_field + 1]
    signal_velocity = jnp.maximum(jnp.abs(advected_field_left), jnp.abs(advected_field_right))
    interface_fluxes = 0.5 * (advected_field_left * state_left_side + advected_field_right * state_right_side) - 0.5 * signal_velocity * (state_right_side - state_left_side)
    return lax.slice_in_dim(interface_fluxes, 1, extent - 3, axis=sweep_direction) - lax.slice_in_dim(interface_fluxes, 0, extent - 4, axis=sweep_direction)

def advance(halo_extended_field):
    centre = halo_extended_field[:, :, 2:-2]
    lat_div = flux_divergence(halo_extended_field, 2, 1)
    wrapped = jnp.concatenate([centre[..., -2:], centre, centre[..., :2]], axis=3)
    lon_div = flux_divergence(wrapped, 3, 0)
    return centre - COURANT * (lat_div + lon_div)

def obs_space(tile_state, obs_value, obs_site):
    site_count = tile_state.shape[2]
    ens_mean = lax.optimization_barrier(jnp.mean(tile_state, axis=1))
    anomaly = tile_state - ens_mean[:, None, :]
    selector = (obs_site[:, :, None] == jnp.arange(site_count)[None, None, :]).astype(jnp.float32)
    obs_anomaly = jnp.einsum('bos,bks->bok', selector, anomaly, precision=HIGHEST)
    obs_mean = jnp.einsum('bos,bs->bo', selector, ens_mean, precision=HIGHEST)
    return (ens_mean, anomaly, obs_anomaly, obs_value - obs_mean)

def transform(local_anomaly, local_innovation, local_weight, ens_mean, anomaly):
    members = local_anomaly.shape[2]
    identity = jnp.eye(members, dtype=jnp.float32)
    weighted = local_anomaly * local_weight[:, :, None]
    gram_matrix = jnp.einsum('bpk,bpj->bkj', weighted, local_anomaly, precision=HIGHEST) + (members - 1.0) * identity
    frob_norm = jnp.sqrt(lax.optimization_barrier(jnp.sum(gram_matrix * gram_matrix, axis=(1, 2))))
    root_iter = gram_matrix / frob_norm[:, None, None]
    inverse = jnp.broadcast_to(identity, gram_matrix.shape)
    for sweep in range(NSI):
        factor = 1.5 * identity - 0.5 * jnp.matmul(inverse, root_iter, precision=HIGHEST)
        root_iter = jnp.matmul(root_iter, factor, precision=HIGHEST)
        inverse = jnp.matmul(factor, inverse, precision=HIGHEST)
    projected = jnp.einsum('bpk,bp->bk', weighted, local_innovation, precision=HIGHEST)
    halfway = jnp.einsum('bkj,bj->bk', inverse, projected, precision=HIGHEST)
    mean_weights = jnp.einsum('bkj,bj->bk', inverse, halfway, precision=HIGHEST) / frob_norm[:, None]
    spread_weights = inverse * jnp.sqrt((members - 1.0) / frob_norm)[:, None, None]
    combined = spread_weights + mean_weights[:, :, None]
    return ens_mean[:, None, :] + jnp.einsum('bjk,bjs->bks', combined, anomaly, precision=HIGHEST)

def localise(obs_anomaly, innovation, slot_weight, neighbour_tiles, loc_weight, ens_mean, anomaly):
    batch_tiles = neighbour_tiles.shape[0]
    local_anomaly = obs_anomaly[neighbour_tiles].reshape(batch_tiles, -1, obs_anomaly.shape[2])
    local_innovation = innovation[neighbour_tiles].reshape(batch_tiles, -1)
    local_weight = (loc_weight[:, :, None] * slot_weight[neighbour_tiles]).reshape(batch_tiles, -1)
    return transform(local_anomaly, local_innovation, local_weight, ens_mean, anomaly)

def reference(ensemble, obs_value, obs_site, obs_count, obs_precision, loc_weight, neighbours):
    fields = ensemble
    for repeat in range(STEPS):
        fields = advance(jnp.pad(fields, ((0, 0), (0, 0), (2, 2), (0, 0))))
    members, variables, lat_total, lon_total = fields.shape
    tile_count = lat_total * lon_total // TILE
    tile_state = fields.reshape(members, variables, tile_count, TILE).transpose(2, 0, 1, 3).reshape(tile_count, members, variables * TILE)
    block_size = math.gcd(tile_count, 64)

    def blocked(array):
        return array.reshape((tile_count // block_size, block_size) + array.shape[1:])

    def unblocked(array):
        return array.reshape((tile_count,) + array.shape[2:])

    def space_block(parts):
        return obs_space(parts[0], parts[1], parts[2])
    results = lax.map(space_block, (blocked(tile_state), blocked(obs_value), blocked(obs_site)))
    ens_mean, anomaly, obs_anomaly, innovation = [unblocked(item) for item in results]
    live_slots = jnp.arange(obs_value.shape[1]).astype(jnp.int32)[None, :] < obs_count[:, None]
    slot_weight = jnp.where(live_slots, obs_precision, 0.0)
    neighbour_tiles = (jnp.arange(tile_count) // TILES_A * TILES_A).astype(jnp.int32)[:, None] + neighbours

    def analyse_block(parts):
        return localise(obs_anomaly, innovation, slot_weight, parts[0], parts[1], parts[2], parts[3])
    analysed = unblocked(lax.map(analyse_block, (blocked(neighbour_tiles), blocked(loc_weight), blocked(ens_mean), blocked(anomaly))))
    fields = analysed.reshape(tile_count, members, variables, TILE).transpose(1, 2, 0, 3).reshape(members, variables, lat_total, lon_total)
    return advance(jnp.pad(fields, ((0, 0), (0, 0), (2, 2), (0, 0))))
```

```python
import jax
import jax.numpy as jnp
from jax import lax
from jax.experimental import pallas as pl
from jax.experimental.pallas import tpu as pltpu
from jax.sharding import Mesh, PartitionSpec as P

NSI = 6
STEPS = 2
COURANT = 0.08
HIGHEST = lax.Precision.HIGHEST
MEMBERS = 128
VMEM = pl.BlockSpec(memory_space=pltpu.VMEM)
SMEM = pl.BlockSpec(memory_space=pltpu.SMEM)


def half_minmod(lower, upper):
    return 0.5 * (
        jnp.maximum(0.0, jnp.minimum(lower, upper)) + jnp.minimum(0.0, jnp.maximum(lower, upper))
    )


def twice_flux(left, right, carrier):
    speed = jnp.maximum(jnp.abs(left[carrier]), jnp.abs(right[carrier]))
    gain_left = left[carrier] + speed
    gain_right = right[carrier] - speed
    return [gain_left * l + gain_right * r for l, r in zip(left, right)]


def transport(rows):
    count, variables = len(rows), range(len(rows[0]))
    jumps = [[rows[i + 1][v] - rows[i][v] for v in variables] for i in range(count - 1)]
    halves = [None] + [
        [half_minmod(jumps[i - 1][v], jumps[i][v]) for v in variables] for i in range(1, count - 1)
    ]
    fluxes = [None] + [
        twice_flux(
            [rows[i][v] + halves[i][v] for v in variables],
            [rows[i + 1][v] - halves[i + 1][v] for v in variables],
            1,
        )
        for i in range(1, count - 2)
    ]
    result = []
    for i in range(2, count - 2):
        left, right = [], []
        for v in variables:
            q = rows[i][v]
            jump = pltpu.roll(q, 127, 1) - q
            half = half_minmod(pltpu.roll(jump, 1, 1), jump)
            left.append(q + half)
            right.append(pltpu.roll(q - half, 127, 1))
        flux = twice_flux(left, right, 0)
        result.append(
            [
                rows[i][v]
                - (0.5 * COURANT)
                * ((fluxes[i][v] - fluxes[i - 1][v]) + (flux[v] - pltpu.roll(flux[v], 1, 1)))
                for v in variables
            ]
        )
    return result


def turned(x, groups):
    shift = (16 * groups) % 128
    return pltpu.roll(x, shift, 1) if shift else x


def lanes_of(shape):
    return lax.broadcasted_iota(jnp.int32, shape, 1)


def background_kernel(band_ref, centre_ref, low_ref, high_ref, out_ref):
    def row(ref, r):
        return [ref[pl.ds(v * 4 + r, 8, stride=20), :] for v in range(5)]

    rows = [row(ref, r) for ref in (low_ref, centre_ref, high_ref) for r in range(4)]
    rows = transport(rows)
    keep_low = (band_ref[0] > 0).astype(jnp.float32)
    keep_high = (band_ref[0] < band_ref[1] - 1).astype(jnp.float32)
    for i in (0, 1):
        rows[i] = [x * keep_low for x in rows[i]]
    for i in (6, 7):
        rows[i] = [x * keep_high for x in rows[i]]
    rows = transport(rows)
    lane = lanes_of((8, 128))
    group = lane >> 4
    for q in range(8):
        j = q % 4
        chosen = (q // 4, 2 + q // 4)
        for b in (0, 1):
            slab = None
            for g in range(8):
                u, v = g // 4, g % 4
                piece = turned(rows[chosen[b]][v], g - (2 * j + u))
                slab = piece if slab is None else jnp.where(group == g, piece, slab)
            out_ref[q * 20 + 8 * b : q * 20 + 8 * b + 8, :] = slab
        last = jnp.where(
            lane < 32, turned(rows[chosen[0]][4], -2 * j), turned(rows[chosen[1]][4], 2 - 2 * j)
        )
        out_ref[q * 20 + 16 : q * 20 + 20, :] = jnp.where(
            lane[:4] < 64, last[:4], pltpu.roll(last, 64, 1)[4:]
        )


def statistics_kernel(count_ref, loc_ref, near_ref, value_ref, site_ref, precision_ref, out_ref):
    slot = lanes_of((1, 128))
    sub = lax.broadcasted_iota(jnp.int32, (8, 128), 0)
    lane = lanes_of((8, 128))
    cell = lax.broadcasted_iota(jnp.int32, (128, 128), 0)
    slab = jnp.zeros((8, 128), jnp.float32)
    last = jnp.zeros((8, 128), jnp.float32)
    for u in (0, 1):
        weight = jnp.where(slot < count_ref[u], precision_ref[u : u + 1, :], 0.0)
        both = jnp.where(sub == 0, weight, jnp.where(sub == 1, weight * value_ref[u : u + 1, :], 0.0))
        site = site_ref[u : u + 1, :]
        in_slab = ((cell & 63) == site) & ((cell >> 6) == u)
        in_last = ((64 + (cell & 15)) == site) & (((cell >> 4) & 1) == u)
        dims = (((1,), (1,)), ((), ()))
        slab += lax.dot_general(
            both, in_slab.astype(jnp.float32), dims, precision=HIGHEST,
            preferred_element_type=jnp.float32,
        )
        last += lax.dot_general(
            both, in_last.astype(jnp.float32), dims, precision=HIGHEST,
            preferred_element_type=jnp.float32,
        )
    out = jnp.where(sub < 2, slab, jnp.where(sub < 4, pltpu.roll(last, 2, 0), 0.0))
    for t in (0, 1):
        gain = []
        for u in (0, 1):
            total = jnp.float32(0.0)
            for n in range(3):
                total += jnp.where(near_ref[t, n] == u, loc_ref[t, n], 0.0)
            gain.append(total)
        out = jnp.where(sub == 4 + t, jnp.where((lane >> 6) == 0, gain[0], gain[1]), out)
        out = jnp.where(sub == 6 + t, jnp.where(((lane >> 4) & 1) == 0, gain[0], gain[1]), out)
    out_ref[...] = out


def dot(a, b):
    return jnp.dot(a, b, precision=HIGHEST, preferred_element_type=jnp.float32)


def analysis_kernel(half_ref, own_ref, other_ref, own_stats_ref, out_ref):
    lane8 = lanes_of((8, 128))
    sub8 = lax.broadcasted_iota(jnp.int32, (8, 128), 0)
    lane = lanes_of((MEMBERS, 128))
    lane1 = lanes_of((1, 128))
    slabs = []
    for b in (0, 1):
        slabs.append(
            jnp.concatenate(
                [
                    ref[s * 20 + 8 * b : s * 20 + 8 * b + 8, :]
                    for ref in (own_ref, other_ref)
                    for s in range(8)
                ],
                axis=0,
            )
        )
    parts = []
    for ref in (own_ref, other_ref):
        for s in range(8):
            four = ref[s * 20 + 16 : s * 20 + 20, :]
            eight = jnp.concatenate([four, four], axis=0)
            eight = jnp.where(sub8 < 4, eight, pltpu.roll(eight, 64, 1))
            parts.append(jnp.where(lane8 < 64, eight, 0.0))
    slabs.append(jnp.concatenate(parts, axis=0))
    means = [jnp.sum(x, axis=0, keepdims=True) * (1.0 / MEMBERS) for x in slabs]
    slabs = [x - m for x, m in zip(slabs, means)]
    first = half_ref[0] == 0
    own = own_stats_ref[...]
    other = other_ref[160:168, :]
    stats = [jnp.where(first, own, other), jnp.where(first, other, own)]
    eye = (lax.broadcasted_iota(jnp.int32, (MEMBERS, 128), 0) == lane).astype(jnp.float32)
    tiles = [(b, t) for b in (0, 1) for t in (0, 1)]
    tops, fields, norms = [], [], []
    for b, t in tiles:
        s = stats[b]
        mine = (lane1 >> 5) == b
        gain = s[4 + t : 5 + t]
        gain_last = jnp.where(mine, s[6 + t : 7 + t], 0.0)
        pull = gain * (s[1:2] - s[0:1] * means[b])
        pull_last = gain_last * (s[3:4] - s[2:3] * means[2])
        p, r = slabs[b], slabs[2]
        gram = lax.dot_general(
            jnp.concatenate([p * (gain * s[0:1]), r * (gain_last * s[2:3])], axis=1),
            jnp.concatenate([p, r], axis=1),
            (((1,), (1,)), ((), ())),
            precision=HIGHEST,
            preferred_element_type=jnp.float32,
        )
        gram = gram + (MEMBERS - 1.0) * eye
        norm = jnp.sqrt(jnp.sum(jnp.sum(gram * gram, axis=0, keepdims=True), axis=1, keepdims=True))
        norms.append(norm)
        tops.append(gram * (1.0 / norm))
        b_col = jnp.sum(p * pull + r * pull_last, axis=1, keepdims=True)
        if t == 0:
            field = jnp.where(
                lane < 64, p, jnp.where((lane >> 4) == 4 + 2 * b, pltpu.roll(r, 64, 1), 0.0)
            )
            field = jnp.where(lane == 127, b_col, field)
        else:
            field = jnp.where(lane >= 64, p, jnp.where((lane >> 4) == 2 * b + 1, r, 0.0))
            field = jnp.where(lane == 0, b_col, field)
        fields.append(field)
    for sweep in range(NSI):
        factors = [1.5 * eye - 0.5 * x for x in tops]
        if sweep < NSI - 1:
            both = [
                dot(f, jnp.concatenate([x, y], axis=1)) for f, x, y in zip(factors, tops, fields)
            ]
            fields = [x[:, 128:] for x in both]
            tops = [dot(x[:, :128], f) for f, x in zip(factors, both)]
        else:
            fields = [dot(f, y) for f, y in zip(factors, fields)]
    moved = []
    for (b, t), field, norm in zip(tiles, fields, norms):
        column = field[:, 127:128] if t == 0 else field[:, 0:1]
        shift = jnp.sum(column * field, axis=0, keepdims=True) * (1.0 / norm)
        moved.append(field[:64] * jnp.sqrt((MEMBERS - 1.0) / norm) + shift)
    lane64 = lanes_of((64, 128))
    outs = [
        jnp.where(lane64 < 64, moved[0], moved[1]) + means[0],
        jnp.where(lane64 < 64, moved[2], moved[3]) + means[1],
    ]
    group = lane64 >> 4
    last = jnp.where(group == 1, moved[1], pltpu.roll(moved[0], 64, 1))
    last = jnp.where(group == 2, pltpu.roll(moved[2], 64, 1), last)
    last = jnp.where(group == 3, moved[3], last) + means[2]
    for d in range(8):
        for b in (0, 1):
            out_ref[d * 20 + 8 * b : d * 20 + 8 * b + 8, :] = outs[b][8 * d : 8 * d + 8]
        piece = last[8 * d : 8 * d + 8]
        out_ref[d * 20 + 16 : d * 20 + 20, :] = jnp.where(
            lane8[:4] < 64, piece[:4], pltpu.roll(piece, 64, 1)[4:]
        )


def unpack_kernel(in_ref, low_ref, high_ref):
    lane = lanes_of((8, 128))
    sub = lax.broadcasted_iota(jnp.int32, (8, 128), 0)
    group = lane >> 4
    lasts = []
    for q in range(8):
        four = in_ref[q * 20 + 16 : q * 20 + 20, :]
        eight = jnp.concatenate([four, four], axis=0)
        lasts.append(jnp.where(sub < 4, eight, pltpu.roll(eight, 64, 1)))
    for r in range(4):
        b, out_ref = r // 2, (low_ref if r < 2 else high_ref)
        for v in range(5):
            field = None
            for j in range(4):
                q = (r % 2) * 4 + j
                if v < 4:
                    slab = in_ref[q * 20 + 8 * b : q * 20 + 8 * b + 8, :]
                    for u in (0, 1):
                        piece = turned(slab, 2 * j + u - 4 * u - v)
                        field = piece if field is None else jnp.where(group == 2 * j + u, piece, field)
                else:
                    piece = turned(lasts[q], 2 * j - 2 * b)
                    field = piece if field is None else jnp.where((group >> 1) == j, piece, field)
            at = (v * 2 + r % 2) * 8
            out_ref[at : at + 8, :] = field


def forecast_kernel(below_ref, low_ref, high_ref, above_ref, out_ref):
    def row(ref, r):
        return [ref[(v * 2 + r) * 8 : (v * 2 + r) * 8 + 8, :] for v in range(5)]

    rows = [row(ref, r) for ref in (below_ref, low_ref, high_ref, above_ref) for r in (0, 1)]
    rows = transport(rows)
    for r in range(4):
        for v in range(5):
            out_ref[pl.ds(v * 4 + r, 8, stride=20), :] = rows[r][v]


def array(*shape):
    return jax.ShapeDtypeStruct(shape, jnp.float32)


def shards(ensemble, obs_value, obs_site, obs_count, obs_precision, loc_weight, neighbours):
    bands = lax.axis_size("band")
    forward = [(i, i + 1) for i in range(bands - 1)]
    backward = [(target, source) for source, target in forward]
    here = jnp.stack([lax.axis_index("band"), jnp.int32(bands)])
    fields = ensemble.reshape(160, 128)
    low = lax.ppermute(fields, "band", forward)
    high = lax.ppermute(fields, "band", backward)
    stats = pl.pallas_call(
        statistics_kernel,
        out_shape=array(8, 128),
        in_specs=[SMEM] * 3 + [VMEM] * 3,
        out_specs=VMEM,
        name="statistics",
    )(obs_count, loc_weight, neighbours, obs_value, obs_site, obs_precision)
    packed = pl.pallas_call(
        background_kernel,
        out_shape=array(160, 128),
        in_specs=[SMEM] + [VMEM] * 3,
        out_specs=VMEM,
        name="background",
    )(here, fields, low, high)
    own = lax.all_to_all(packed.reshape(8, 5, 4, 128), "q", split_axis=0, concat_axis=0, tiled=True)
    own = own.reshape(160, 128)
    other = lax.ppermute(jnp.concatenate([own, stats], axis=0), "half", [(0, 1), (1, 0)])
    analysed = pl.pallas_call(
        analysis_kernel,
        out_shape=array(160, 128),
        in_specs=[SMEM] + [VMEM] * 3,
        out_specs=VMEM,
        name="analysis",
    )(jnp.reshape(lax.axis_index("half"), (1,)), own, other, stats)
    returned = lax.all_to_all(
        analysed.reshape(8, 5, 4, 128), "q", split_axis=0, concat_axis=0, tiled=True
    )
    low, high = pl.pallas_call(
        unpack_kernel,
        out_shape=(array(80, 128), array(80, 128)),
        in_specs=[VMEM],
        out_specs=(VMEM, VMEM),
        name="unpack",
    )(returned.reshape(160, 128))
    below = lax.ppermute(high, "band", forward)
    above = lax.ppermute(low, "band", backward)
    out = pl.pallas_call(
        forecast_kernel,
        out_shape=array(160, 128),
        in_specs=[VMEM] * 4,
        out_specs=VMEM,
        name="forecast",
    )(below, low, high, above)
    return out.reshape(8, 5, 4, 128)


def solution(mesh):
    bands = mesh.shape["band"]
    fine = Mesh(mesh.devices.reshape(bands, 2, 8), ("band", "half", "q"))
    members = ("half", "q")
    tiles = ("band", "half", "q")
    return jax.shard_map(
        shards,
        mesh=fine,
        in_specs=(
            P(members, None, "band", None),
            P(tiles, None),
            P(tiles, None),
            P(tiles),
            P(tiles, None),
            P(tiles, None),
            P(tiles, None),
        ),
        out_specs=P(members, None, "band", None),
        check_vma=False,
    )
```

```python
import jax
import jax.numpy as jnp
from jax import lax
from jax.experimental import pallas as pl
from jax.experimental.pallas import tpu as pltpu
from jax.sharding import Mesh, PartitionSpec as P

NSI = 6
STEPS = 2
COURANT = 0.08
HIGHEST = lax.Precision.HIGHEST
MEMBERS = 128
VMEM = pl.BlockSpec(memory_space=pltpu.VMEM)
SMEM = pl.BlockSpec(memory_space=pltpu.SMEM)
SMALL = pltpu.CompilerParams(vmem_limit_bytes=8 * 2**20)


def half_minmod(lower, upper):
    return 0.5 * (
        jnp.maximum(0.0, jnp.minimum(lower, upper)) + jnp.minimum(0.0, jnp.maximum(lower, upper))
    )


def twice_flux(left, right, carrier):
    speed = jnp.maximum(jnp.abs(left[carrier]), jnp.abs(right[carrier]))
    gain_left = left[carrier] + speed
    gain_right = right[carrier] - speed
    return [gain_left * l + gain_right * r for l, r in zip(left, right)]


def transport(rows):
    count, variables = len(rows), range(len(rows[0]))
    jumps = [[rows[i + 1][v] - rows[i][v] for v in variables] for i in range(count - 1)]
    halves = [None] + [
        [half_minmod(jumps[i - 1][v], jumps[i][v]) for v in variables] for i in range(1, count - 1)
    ]
    fluxes = [None] + [
        twice_flux(
            [rows[i][v] + halves[i][v] for v in variables],
            [rows[i + 1][v] - halves[i + 1][v] for v in variables],
            1,
        )
        for i in range(1, count - 2)
    ]
    result = []
    for i in range(2, count - 2):
        left, right = [], []
        for v in variables:
            q = rows[i][v]
            jump = pltpu.roll(q, 127, 1) - q
            half = half_minmod(pltpu.roll(jump, 1, 1), jump)
            left.append(q + half)
            right.append(pltpu.roll(q - half, 127, 1))
        flux = twice_flux(left, right, 0)
        result.append(
            [
                rows[i][v]
                - (0.5 * COURANT)
                * ((fluxes[i][v] - fluxes[i - 1][v]) + (flux[v] - pltpu.roll(flux[v], 1, 1)))
                for v in variables
            ]
        )
    return result


def turned(x, groups):
    shift = (16 * groups) % 128
    return pltpu.roll(x, shift, 1) if shift else x


def lanes_of(shape):
    return lax.broadcasted_iota(jnp.int32, shape, 1)


def background_kernel(band_ref, centre_ref, low_ref, high_ref, out_ref):
    def row(ref, r):
        return [ref[pl.ds(v * 4 + r, 8, stride=20), :] for v in range(5)]

    rows = [row(ref, r) for ref in (low_ref, centre_ref, high_ref) for r in range(4)]
    rows = transport(rows)
    keep_low = (band_ref[0] > 0).astype(jnp.float32)
    keep_high = (band_ref[0] < band_ref[1] - 1).astype(jnp.float32)
    for i in (0, 1):
        rows[i] = [x * keep_low for x in rows[i]]
    for i in (6, 7):
        rows[i] = [x * keep_high for x in rows[i]]
    rows = transport(rows)
    lane = lanes_of((8, 128))
    group = lane >> 4
    for q in range(8):
        j = q % 4
        chosen = (q // 4, 2 + q // 4)
        for b in (0, 1):
            slab = None
            for g in range(8):
                u, v = g // 4, g % 4
                piece = turned(rows[chosen[b]][v], g - (2 * j + u))
                slab = piece if slab is None else jnp.where(group == g, piece, slab)
            out_ref[q * 20 + 8 * b : q * 20 + 8 * b + 8, :] = slab
        last = jnp.where(
            lane < 32, turned(rows[chosen[0]][4], -2 * j), turned(rows[chosen[1]][4], 2 - 2 * j)
        )
        out_ref[q * 20 + 16 : q * 20 + 20, :] = jnp.where(
            lane[:4] < 64, last[:4], pltpu.roll(last, 64, 1)[4:]
        )


def statistics_kernel(count_ref, loc_ref, near_ref, value_ref, site_ref, precision_ref, out_ref):
    slot = lanes_of((1, 128))
    sub = lax.broadcasted_iota(jnp.int32, (8, 128), 0)
    lane = lanes_of((8, 128))
    cell = lax.broadcasted_iota(jnp.int32, (128, 128), 0)
    slab = jnp.zeros((8, 128), jnp.float32)
    last = jnp.zeros((8, 128), jnp.float32)
    for u in (0, 1):
        weight = jnp.where(slot < count_ref[u], precision_ref[u : u + 1, :], 0.0)
        both = jnp.where(sub == 0, weight, jnp.where(sub == 1, weight * value_ref[u : u + 1, :], 0.0))
        site = site_ref[u : u + 1, :]
        in_slab = ((cell & 63) == site) & ((cell >> 6) == u)
        in_last = ((64 + (cell & 15)) == site) & (((cell >> 4) & 1) == u)
        dims = (((1,), (1,)), ((), ()))
        slab += lax.dot_general(
            both, in_slab.astype(jnp.float32), dims, precision=HIGHEST,
            preferred_element_type=jnp.float32,
        )
        last += lax.dot_general(
            both, in_last.astype(jnp.float32), dims, precision=HIGHEST,
            preferred_element_type=jnp.float32,
        )
    out = jnp.where(sub < 2, slab, jnp.where(sub < 4, pltpu.roll(last, 2, 0), 0.0))
    for t in (0, 1):
        gain = []
        for u in (0, 1):
            total = jnp.float32(0.0)
            for n in range(3):
                total += jnp.where(near_ref[t, n] == u, loc_ref[t, n], 0.0)
            gain.append(total)
        out = jnp.where(sub == 4 + t, jnp.where((lane >> 6) == 0, gain[0], gain[1]), out)
        out = jnp.where(sub == 6 + t, jnp.where(((lane >> 4) & 1) == 0, gain[0], gain[1]), out)
    out_ref[...] = out


def dot(a, b):
    return jnp.dot(a, b, precision=HIGHEST, preferred_element_type=jnp.float32)


def analysis_kernel(half_ref, own_ref, other_ref, own_stats_ref, out_ref):
    lane8 = lanes_of((8, 128))
    sub8 = lax.broadcasted_iota(jnp.int32, (8, 128), 0)
    lane = lanes_of((MEMBERS, 128))
    lane1 = lanes_of((1, 128))
    slabs = []
    for b in (0, 1):
        slabs.append(
            jnp.concatenate(
                [
                    ref[s * 20 + 8 * b : s * 20 + 8 * b + 8, :]
                    for ref in (own_ref, other_ref)
                    for s in range(8)
                ],
                axis=0,
            )
        )
    parts = []
    for ref in (own_ref, other_ref):
        for s in range(8):
            four = ref[s * 20 + 16 : s * 20 + 20, :]
            eight = jnp.concatenate([four, four], axis=0)
            eight = jnp.where(sub8 < 4, eight, pltpu.roll(eight, 64, 1))
            parts.append(jnp.where(lane8 < 64, eight, 0.0))
    slabs.append(jnp.concatenate(parts, axis=0))
    means = [jnp.sum(x, axis=0, keepdims=True) * (1.0 / MEMBERS) for x in slabs]
    slabs = [x - m for x, m in zip(slabs, means)]
    first = half_ref[0] == 0
    own = own_stats_ref[...]
    other = other_ref[160:168, :]
    stats = [jnp.where(first, own, other), jnp.where(first, other, own)]
    eye = (lax.broadcasted_iota(jnp.int32, (MEMBERS, 128), 0) == lane).astype(jnp.float32)
    tiles = [(b, t) for b in (0, 1) for t in (0, 1)]
    tops, fields, norms = [], [], []
    for b, t in tiles:
        s = stats[b]
        mine = (lane1 >> 5) == b
        gain = s[4 + t : 5 + t]
        gain_last = jnp.where(mine, s[6 + t : 7 + t], 0.0)
        pull = gain * (s[1:2] - s[0:1] * means[b])
        pull_last = gain_last * (s[3:4] - s[2:3] * means[2])
        p, r = slabs[b], slabs[2]
        gram = lax.dot_general(
            jnp.concatenate([p * (gain * s[0:1]), r * (gain_last * s[2:3])], axis=1),
            jnp.concatenate([p, r], axis=1),
            (((1,), (1,)), ((), ())),
            precision=HIGHEST,
            preferred_element_type=jnp.float32,
        )
        gram = gram + (MEMBERS - 1.0) * eye
        norm = jnp.sqrt(jnp.sum(jnp.sum(gram * gram, axis=0, keepdims=True), axis=1, keepdims=True))
        norms.append(norm)
        tops.append(gram * (1.0 / norm))
        b_col = jnp.sum(p * pull + r * pull_last, axis=1, keepdims=True)
        if t == 0:
            field = jnp.where(
                lane < 64, p, jnp.where((lane >> 4) == 4 + 2 * b, pltpu.roll(r, 64, 1), 0.0)
            )
            field = jnp.where(lane == 127, b_col, field)
        else:
            field = jnp.where(lane >= 64, p, jnp.where((lane >> 4) == 2 * b + 1, r, 0.0))
            field = jnp.where(lane == 0, b_col, field)
        fields.append(field)
    for sweep in range(NSI):
        factors = [1.5 * eye - 0.5 * x for x in tops]
        if sweep < NSI - 1:
            both = [
                dot(f, jnp.concatenate([x, y], axis=1)) for f, x, y in zip(factors, tops, fields)
            ]
            fields = [x[:, 128:] for x in both]
            tops = [dot(x[:, :128], f) for f, x in zip(factors, both)]
        else:
            fields = [dot(f, y) for f, y in zip(factors, fields)]
    moved = []
    for (b, t), field, norm in zip(tiles, fields, norms):
        column = field[:, 127:128] if t == 0 else field[:, 0:1]
        shift = jnp.sum(column * field, axis=0, keepdims=True) * (1.0 / norm)
        moved.append(field[:64] * jnp.sqrt((MEMBERS - 1.0) / norm) + shift)
    lane64 = lanes_of((64, 128))
    outs = [
        jnp.where(lane64 < 64, moved[0], moved[1]) + means[0],
        jnp.where(lane64 < 64, moved[2], moved[3]) + means[1],
    ]
    group = lane64 >> 4
    last = jnp.where(group == 1, moved[1], pltpu.roll(moved[0], 64, 1))
    last = jnp.where(group == 2, pltpu.roll(moved[2], 64, 1), last)
    last = jnp.where(group == 3, moved[3], last) + means[2]
    for d in range(8):
        for b in (0, 1):
            out_ref[d * 20 + 8 * b : d * 20 + 8 * b + 8, :] = outs[b][8 * d : 8 * d + 8]
        piece = last[8 * d : 8 * d + 8]
        out_ref[d * 20 + 16 : d * 20 + 20, :] = jnp.where(
            lane8[:4] < 64, piece[:4], pltpu.roll(piece, 64, 1)[4:]
        )


def unpack_kernel(in_ref, low_ref, high_ref):
    lane = lanes_of((8, 128))
    sub = lax.broadcasted_iota(jnp.int32, (8, 128), 0)
    group = lane >> 4
    lasts = []
    for q in range(8):
        four = in_ref[q * 20 + 16 : q * 20 + 20, :]
        eight = jnp.concatenate([four, four], axis=0)
        lasts.append(jnp.where(sub < 4, eight, pltpu.roll(eight, 64, 1)))
    for r in range(4):
        b, out_ref = r // 2, (low_ref if r < 2 else high_ref)
        for v in range(5):
            field = None
            for j in range(4):
                q = (r % 2) * 4 + j
                if v < 4:
                    slab = in_ref[q * 20 + 8 * b : q * 20 + 8 * b + 8, :]
                    for u in (0, 1):
                        piece = turned(slab, 2 * j + u - 4 * u - v)
                        field = piece if field is None else jnp.where(group == 2 * j + u, piece, field)
                else:
                    piece = turned(lasts[q], 2 * j - 2 * b)
                    field = piece if field is None else jnp.where((group >> 1) == j, piece, field)
            at = (v * 2 + r % 2) * 8
            out_ref[at : at + 8, :] = field


def forecast_kernel(below_ref, low_ref, high_ref, above_ref, out_ref):
    def row(ref, r):
        return [ref[(v * 2 + r) * 8 : (v * 2 + r) * 8 + 8, :] for v in range(5)]

    rows = [row(ref, r) for ref in (below_ref, low_ref, high_ref, above_ref) for r in (0, 1)]
    rows = transport(rows)
    for r in range(4):
        for v in range(5):
            out_ref[pl.ds(v * 4 + r, 8, stride=20), :] = rows[r][v]


def array(*shape):
    return jax.ShapeDtypeStruct(shape, jnp.float32)


def shards(ensemble, obs_value, obs_site, obs_count, obs_precision, loc_weight, neighbours):
    bands = lax.axis_size("band")
    forward = [(i, i + 1) for i in range(bands - 1)]
    backward = [(target, source) for source, target in forward]
    here = jnp.stack([lax.axis_index("band"), jnp.int32(bands)])
    fields = ensemble.reshape(160, 128)
    low = lax.ppermute(fields, "band", forward)
    high = lax.ppermute(fields, "band", backward)
    stats = pl.pallas_call(
        statistics_kernel,
        out_shape=array(8, 128),
        in_specs=[SMEM] * 3 + [VMEM] * 3,
        out_specs=VMEM,
        compiler_params=SMALL,
        name="statistics",
    )(obs_count, loc_weight, neighbours, obs_value, obs_site, obs_precision)
    packed = pl.pallas_call(
        background_kernel,
        out_shape=array(160, 128),
        in_specs=[SMEM] + [VMEM] * 3,
        out_specs=VMEM,
        compiler_params=SMALL,
        name="background",
    )(here, fields, low, high)
    own = lax.all_to_all(packed.reshape(8, 5, 4, 128), "q", split_axis=0, concat_axis=0, tiled=True)
    own = own.reshape(160, 128)
    other = lax.ppermute(jnp.concatenate([own, stats], axis=0), "half", [(0, 1), (1, 0)])
    analysed = pl.pallas_call(
        analysis_kernel,
        out_shape=array(160, 128),
        in_specs=[SMEM] + [VMEM] * 3,
        out_specs=VMEM,
        compiler_params=SMALL,
        name="analysis",
    )(jnp.reshape(lax.axis_index("half"), (1,)), own, other, stats)
    returned = lax.all_to_all(
        analysed.reshape(8, 5, 4, 128), "q", split_axis=0, concat_axis=0, tiled=True
    )
    low, high = pl.pallas_call(
        unpack_kernel,
        out_shape=(array(80, 128), array(80, 128)),
        in_specs=[VMEM],
        out_specs=(VMEM, VMEM),
        compiler_params=SMALL,
        name="unpack",
    )(returned.reshape(160, 128))
    below = lax.ppermute(high, "band", forward)
    above = lax.ppermute(low, "band", backward)
    out = pl.pallas_call(
        forecast_kernel,
        out_shape=array(160, 128),
        in_specs=[VMEM] * 4,
        out_specs=VMEM,
        compiler_params=SMALL,
        name="forecast",
    )(below, low, high, above)
    return out.reshape(8, 5, 4, 128)


def solution(mesh):
    bands = mesh.shape["band"]
    fine = Mesh(mesh.devices.reshape(bands, 2, 8), ("band", "half", "q"))
    members = ("half", "q")
    tiles = ("band", "half", "q")
    return jax.shard_map(
        shards,
        mesh=fine,
        in_specs=(
            P(members, None, "band", None),
            P(tiles, None),
            P(tiles, None),
            P(tiles),
            P(tiles, None),
            P(tiles, None),
            P(tiles, None),
        ),
        out_specs=P(members, None, "band", None),
        check_vma=False,
    )
```

```python
import jax
import jax.numpy as jnp
from jax import lax
from jax.experimental import pallas as pl
from jax.experimental.pallas import tpu as pltpu
from jax.sharding import Mesh, PartitionSpec as P

NSI = 6
COURANT = 0.08
HIGHEST = lax.Precision.HIGHEST
MEMBERS = 128
VMEM = pl.BlockSpec(memory_space=pltpu.VMEM)
HBM = pl.BlockSpec(memory_space=pltpu.HBM)
SMEM = pl.BlockSpec(memory_space=pltpu.SMEM)
LARGE = pltpu.CompilerParams(vmem_limit_bytes=60 * 2**20)
SMALL = pltpu.CompilerParams(vmem_limit_bytes=8 * 2**20)


def half_minmod(lower, upper):
    return 0.5 * (
        jnp.maximum(0.0, jnp.minimum(lower, upper)) + jnp.minimum(0.0, jnp.maximum(lower, upper))
    )


def twice_flux(left, right, carrier):
    speed = jnp.maximum(jnp.abs(left[carrier]), jnp.abs(right[carrier]))
    gain_left = left[carrier] + speed
    gain_right = right[carrier] - speed
    return [gain_left * l + gain_right * r for l, r in zip(left, right)]


def transport(rows):
    count, variables = len(rows), range(len(rows[0]))
    jumps = [[rows[i + 1][v] - rows[i][v] for v in variables] for i in range(count - 1)]
    halves = [None] + [
        [half_minmod(jumps[i - 1][v], jumps[i][v]) for v in variables] for i in range(1, count - 1)
    ]
    fluxes = [None] + [
        twice_flux(
            [rows[i][v] + halves[i][v] for v in variables],
            [rows[i + 1][v] - halves[i + 1][v] for v in variables],
            1,
        )
        for i in range(1, count - 2)
    ]
    result = []
    for i in range(2, count - 2):
        left, right = [], []
        for v in variables:
            q = rows[i][v]
            jump = pltpu.roll(q, 127, 1) - q
            half = half_minmod(pltpu.roll(jump, 1, 1), jump)
            left.append(q + half)
            right.append(pltpu.roll(q - half, 127, 1))
        flux = twice_flux(left, right, 0)
        result.append(
            [
                rows[i][v]
                - (0.5 * COURANT)
                * ((fluxes[i][v] - fluxes[i - 1][v]) + (flux[v] - pltpu.roll(flux[v], 1, 1)))
                for v in variables
            ]
        )
    return result


def turned(x, groups):
    shift = (16 * groups) % 128
    return pltpu.roll(x, shift, 1) if shift else x


def lanes_of(shape):
    return lax.broadcasted_iota(jnp.int32, shape, 1)


def background(band_ref, centre_ref, low_ref, high_ref, out_ref, offset):
    def row(ref, r):
        return [ref[pl.ds(v * 4 + r, 8, stride=20), :] for v in range(5)]

    rows = [row(ref, r) for ref in (low_ref, centre_ref, high_ref) for r in range(4)]
    rows = transport(rows)
    keep_low = (band_ref[0] > 0).astype(jnp.float32)
    keep_high = (band_ref[0] < band_ref[1] - 1).astype(jnp.float32)
    for i in (0, 1):
        rows[i] = [x * keep_low for x in rows[i]]
    for i in (6, 7):
        rows[i] = [x * keep_high for x in rows[i]]
    rows = transport(rows)
    lane = lanes_of((8, 128))
    group = lane >> 4
    for q in range(8):
        j = q % 4
        at = q * 40 + offset
        chosen = (q // 4, 2 + q // 4)
        for b in (0, 1):
            slab = None
            for g in range(8):
                u, v = g // 4, g % 4
                piece = turned(rows[chosen[b]][v], g - (2 * j + u))
                slab = piece if slab is None else jnp.where(group == g, piece, slab)
            out_ref[at + 8 * b : at + 8 * b + 8, :] = slab
        last = jnp.where(
            lane < 32, turned(rows[chosen[0]][4], -2 * j), turned(rows[chosen[1]][4], 2 - 2 * j)
        )
        out_ref[at + 16 : at + 20, :] = jnp.where(
            lane[:4] < 64, last[:4], pltpu.roll(last, 64, 1)[4:]
        )


def own_background_kernel(band_ref, centre_ref, low_ref, high_ref, out_ref):
    background(band_ref, centre_ref, low_ref, high_ref, out_ref, 0)


def other_background_kernel(band_ref, centre_ref, low_ref, high_ref, own_ref, out_ref):
    for q in range(8):
        out_ref[q * 40 : q * 40 + 20, :] = own_ref[q * 40 : q * 40 + 20, :]
    background(band_ref, centre_ref, low_ref, high_ref, out_ref, 20)


def head_kernel(*refs):
    sources, out_ref, targets, arrived = refs[:7], refs[7], refs[8:14], refs[14]
    fields = pltpu.make_async_copy(sources[0], out_ref.at[0:160, :], arrived.at[0])
    fields.start()
    rest = [
        pltpu.make_async_copy(source, target, arrived.at[n + 1])
        for n, (source, target) in enumerate(zip(sources[1:], targets))
    ]
    for copy in rest:
        copy.start()
    for copy in rest:
        copy.wait()
    count_ref, loc_ref, near_ref, value_ref, site_ref, precision_ref = targets
    slot = lanes_of((1, 128))
    out_ref[160:162, :] = value_ref[...]
    out_ref[162:164, :] = site_ref[...].astype(jnp.float32)
    for u in (0, 1):
        out_ref[164 + u : 165 + u, :] = jnp.where(
            slot < count_ref[u], precision_ref[u : u + 1, :], 0.0
        )
    for t in (0, 1):
        gain = []
        for u in (0, 1):
            total = jnp.float32(0.0)
            for n in range(3):
                total += jnp.where(near_ref[t, n] == u, loc_ref[t, n], 0.0)
            gain.append(total)
        out_ref[166 + t : 167 + t, :] = jnp.where(slot < 64, gain[0], gain[1])
    fields.wait()


def statistics_kernel(own_ref, other_ref, out_ref):
    sub = lax.broadcasted_iota(jnp.int32, (8, 128), 0)
    lane = lanes_of((8, 128))
    cell = lax.broadcasted_iota(jnp.int32, (128, 128), 0)
    dims = (((1,), (1,)), ((), ()))
    for k, ref in enumerate((own_ref, other_ref)):
        slab = jnp.zeros((8, 128), jnp.float32)
        last = jnp.zeros((8, 128), jnp.float32)
        for u in (0, 1):
            value = ref[160 + u : 161 + u, :]
            site = ref[162 + u : 163 + u, :].astype(jnp.int32)
            weight = ref[164 + u : 165 + u, :]
            both = jnp.where(sub == 0, weight, jnp.where(sub == 1, weight * value, 0.0))
            in_slab = ((cell & 63) == site) & ((cell >> 6) == u)
            in_last = ((64 + (cell & 15)) == site) & (((cell >> 4) & 1) == u)
            slab += lax.dot_general(
                both, in_slab.astype(jnp.float32), dims, precision=HIGHEST,
                preferred_element_type=jnp.float32,
            )
            last += lax.dot_general(
                both, in_last.astype(jnp.float32), dims, precision=HIGHEST,
                preferred_element_type=jnp.float32,
            )
        out = jnp.where(sub < 2, slab, jnp.where(sub < 4, pltpu.roll(last, 2, 0), 0.0))
        for t in (0, 1):
            gain = ref[166 + t : 167 + t, :]
            out = jnp.where(sub == 4 + t, gain, out)
            gain = jnp.where(((lane >> 4) & 1) == 0, gain[:, 0:1], gain[:, 64:65])
            out = jnp.where(sub == 6 + t, gain, out)
        out_ref[8 * k : 8 * k + 8, :] = out


def dot(a, b):
    return jnp.dot(a, b, precision=HIGHEST, preferred_element_type=jnp.float32)


def analysis_kernel(half_ref, in_ref, stats_ref, out_ref):
    lane8 = lanes_of((8, 128))
    sub8 = lax.broadcasted_iota(jnp.int32, (8, 128), 0)
    lane = lanes_of((MEMBERS, 128))
    lane1 = lanes_of((1, 128))
    slabs = []
    for b in (0, 1):
        slabs.append(
            jnp.concatenate(
                [
                    in_ref[s * 40 + start + 8 * b : s * 40 + start + 8 * b + 8, :]
                    for start in (0, 20)
                    for s in range(8)
                ],
                axis=0,
            )
        )
    parts = []
    for start in (0, 20):
        for s in range(8):
            four = in_ref[s * 40 + start + 16 : s * 40 + start + 20, :]
            eight = jnp.concatenate([four, four], axis=0)
            eight = jnp.where(sub8 < 4, eight, pltpu.roll(eight, 64, 1))
            parts.append(jnp.where(lane8 < 64, eight, 0.0))
    slabs.append(jnp.concatenate(parts, axis=0))
    means = [jnp.sum(x, axis=0, keepdims=True) * (1.0 / MEMBERS) for x in slabs]
    slabs = [x - m for x, m in zip(slabs, means)]
    first = half_ref[0] == 0
    own = stats_ref[0:8, :]
    other = stats_ref[8:16, :]
    stats = [jnp.where(first, own, other), jnp.where(first, other, own)]
    eye = (lax.broadcasted_iota(jnp.int32, (MEMBERS, 128), 0) == lane).astype(jnp.float32)
    tiles = [(b, t) for b in (0, 1) for t in (0, 1)]
    tops, fields, norms = [], [], []
    for b, t in tiles:
        s = stats[b]
        mine = (lane1 >> 5) == b
        gain = s[4 + t : 5 + t]
        gain_last = jnp.where(mine, s[6 + t : 7 + t], 0.0)
        pull = gain * (s[1:2] - s[0:1] * means[b])
        pull_last = gain_last * (s[3:4] - s[2:3] * means[2])
        p, r = slabs[b], slabs[2]
        gram = lax.dot_general(
            jnp.concatenate([p * (gain * s[0:1]), r * (gain_last * s[2:3])], axis=1),
            jnp.concatenate([p, r], axis=1),
            (((1,), (1,)), ((), ())),
            precision=HIGHEST,
            preferred_element_type=jnp.float32,
        )
        gram = gram + (MEMBERS - 1.0) * eye
        norm = jnp.sqrt(jnp.sum(jnp.sum(gram * gram, axis=0, keepdims=True), axis=1, keepdims=True))
        norms.append(norm)
        tops.append(gram * (1.0 / norm))
        b_col = jnp.sum(p * pull + r * pull_last, axis=1, keepdims=True)
        if t == 0:
            field = jnp.where(
                lane < 64, p, jnp.where((lane >> 4) == 4 + 2 * b, pltpu.roll(r, 64, 1), 0.0)
            )
            field = jnp.where(lane == 127, b_col, field)
        else:
            field = jnp.where(lane >= 64, p, jnp.where((lane >> 4) == 2 * b + 1, r, 0.0))
            field = jnp.where(lane == 0, b_col, field)
        fields.append(field)
    for sweep in range(NSI):
        factors = [1.5 * eye - 0.5 * x for x in tops]
        if sweep < NSI - 1:
            both = [
                dot(f, jnp.concatenate([x, y], axis=1)) for f, x, y in zip(factors, tops, fields)
            ]
            fields = [x[:, 128:] for x in both]
            tops = [dot(x[:, :128], f) for f, x in zip(factors, both)]
        else:
            fields = [dot(f, y) for f, y in zip(factors, fields)]
    moved = []
    for (b, t), field, norm in zip(tiles, fields, norms):
        column = field[:, 127:128] if t == 0 else field[:, 0:1]
        shift = jnp.sum(column * field, axis=0, keepdims=True) * (1.0 / norm)
        moved.append(field[:64] * jnp.sqrt((MEMBERS - 1.0) / norm) + shift)
    lane64 = lanes_of((64, 128))
    outs = [
        jnp.where(lane64 < 64, moved[0], moved[1]) + means[0],
        jnp.where(lane64 < 64, moved[2], moved[3]) + means[1],
    ]
    group = lane64 >> 4
    last = jnp.where(group == 1, moved[1], pltpu.roll(moved[0], 64, 1))
    last = jnp.where(group == 2, pltpu.roll(moved[2], 64, 1), last)
    last = jnp.where(group == 3, moved[3], last) + means[2]
    for d in range(8):
        for b in (0, 1):
            out_ref[d * 20 + 8 * b : d * 20 + 8 * b + 8, :] = outs[b][8 * d : 8 * d + 8]
        piece = last[8 * d : 8 * d + 8]
        out_ref[d * 20 + 16 : d * 20 + 20, :] = jnp.where(
            lane8[:4] < 64, piece[:4], pltpu.roll(piece, 64, 1)[4:]
        )


def unpack_kernel(in_ref, low_ref, high_ref):
    lane = lanes_of((8, 128))
    sub = lax.broadcasted_iota(jnp.int32, (8, 128), 0)
    group = lane >> 4
    lasts = []
    for q in range(8):
        four = in_ref[q * 20 + 16 : q * 20 + 20, :]
        eight = jnp.concatenate([four, four], axis=0)
        lasts.append(jnp.where(sub < 4, eight, pltpu.roll(eight, 64, 1)))
    for r in range(4):
        b, out_ref = r // 2, (low_ref if r < 2 else high_ref)
        for v in range(5):
            field = None
            for j in range(4):
                q = (r % 2) * 4 + j
                if v < 4:
                    slab = in_ref[q * 20 + 8 * b : q * 20 + 8 * b + 8, :]
                    for u in (0, 1):
                        piece = turned(slab, 2 * j + u - 4 * u - v)
                        field = piece if field is None else jnp.where(group == 2 * j + u, piece, field)
                else:
                    piece = turned(lasts[q], 2 * j - 2 * b)
                    field = piece if field is None else jnp.where((group >> 1) == j, piece, field)
            at = (v * 2 + r % 2) * 8
            out_ref[at : at + 8, :] = field


def forecast_kernel(below_ref, low_ref, high_ref, above_ref, out_ref):
    def row(ref, r):
        return [ref[(v * 2 + r) * 8 : (v * 2 + r) * 8 + 8, :] for v in range(5)]

    rows = [row(ref, r) for ref in (below_ref, low_ref, high_ref, above_ref) for r in (0, 1)]
    rows = transport(rows)
    for r in range(4):
        for v in range(5):
            out_ref[pl.ds(v * 4 + r, 8, stride=20), :] = rows[r][v]


def array(*shape):
    return jax.ShapeDtypeStruct(shape, jnp.float32)


def call(kernel, name, in_specs, *out, scratch=()):
    return pl.pallas_call(
        kernel,
        out_shape=out if len(out) > 1 else out[0],
        in_specs=in_specs,
        out_specs=(VMEM,) * len(out) if len(out) > 1 else VMEM,
        scratch_shapes=scratch,
        compiler_params=LARGE if name == "head" else SMALL,
    )


def exchange(x):
    return lax.all_to_all(
        x.reshape(8, -1, 4, 128), "q", split_axis=0, concat_axis=0, tiled=True
    ).reshape(x.shape)


def shards(ensemble, obs_value, obs_site, obs_count, obs_precision, loc_weight, neighbours):
    bands = lax.axis_size("band")
    forward = [(i, i + 1) for i in range(bands - 1)]
    backward = [(target, source) for source, target in forward]
    here = jnp.stack([lax.axis_index("band"), jnp.int32(bands)])
    half = jnp.reshape(lax.axis_index("half"), (1,))
    own = call(
        head_kernel, "head", [HBM] * 7, array(168, 128),
        scratch=[
            pltpu.SMEM((2,), jnp.int32),
            pltpu.SMEM((2, 3), jnp.float32),
            pltpu.SMEM((2, 3), jnp.int32),
            pltpu.VMEM((2, 128), jnp.float32),
            pltpu.VMEM((2, 128), jnp.int32),
            pltpu.VMEM((2, 128), jnp.float32),
            pltpu.SemaphoreType.DMA((7,)),
        ],
    )(
        ensemble.reshape(160, 128), obs_count, loc_weight, neighbours,
        obs_value, obs_site, obs_precision,
    )
    other = lax.ppermute(own, "half", [(0, 1), (1, 0)])
    low = lax.ppermute(own, "band", forward)
    high = lax.ppermute(own, "band", backward)
    packed = call(
        own_background_kernel, "own_background", [SMEM] + [VMEM] * 3, array(320, 128)
    )(here, own, low, high)
    low = lax.ppermute(other, "band", forward)
    high = lax.ppermute(other, "band", backward)
    stats = call(statistics_kernel, "statistics", [VMEM] * 2, array(16, 128))(own, other)
    packed = call(
        other_background_kernel, "other_background", [SMEM] + [VMEM] * 4, array(320, 128)
    )(here, other, low, high, packed)
    analysed = call(analysis_kernel, "analysis", [SMEM] + [VMEM] * 2, array(160, 128))(
        half, exchange(packed), stats
    )
    low, high = call(unpack_kernel, "unpack", [VMEM], array(80, 128), array(80, 128))(
        exchange(analysed)
    )
    below = lax.ppermute(high, "band", forward)
    above = lax.ppermute(low, "band", backward)
    out = call(forecast_kernel, "forecast", [VMEM] * 4, array(160, 128))(below, low, high, above)
    return out.reshape(8, 5, 4, 128)


def solution(mesh):
    bands = mesh.shape["band"]
    fine = Mesh(mesh.devices.reshape(bands, 2, 8), ("band", "half", "q"))
    members = ("half", "q")
    tiles = ("band", "half", "q")
    return jax.shard_map(
        shards,
        mesh=fine,
        in_specs=(
            P(members, None, "band", None),
            P(tiles, None),
            P(tiles, None),
            P(tiles),
            P(tiles, None),
            P(tiles, None),
            P(tiles, None),
        ),
        out_specs=P(members, None, "band", None),
        check_vma=False,
    )
```

```python
import functools

import jax
import jax.numpy as jnp
from jax import lax
from jax.experimental import pallas as pl
from jax.experimental.pallas import tpu as pltpu
from jax.sharding import Mesh, PartitionSpec as P

NSI = 6
COURANT = 0.08
HIGHEST = lax.Precision.HIGHEST
MEMBERS = 128
VMEM = pl.BlockSpec(memory_space=pltpu.VMEM)
SMEM = pl.BlockSpec(memory_space=pltpu.SMEM)
SMALL = pltpu.CompilerParams(vmem_limit_bytes=8 * 2**20)


def half_minmod(lower, upper):
    return 0.5 * (
        jnp.maximum(0.0, jnp.minimum(lower, upper)) + jnp.minimum(0.0, jnp.maximum(lower, upper))
    )


def twice_flux(left, right, carrier):
    speed = jnp.maximum(jnp.abs(left[carrier]), jnp.abs(right[carrier]))
    gain_left = left[carrier] + speed
    gain_right = right[carrier] - speed
    return [gain_left * l + gain_right * r for l, r in zip(left, right)]


def transport(rows):
    count, variables = len(rows), range(len(rows[0]))
    jumps = [[rows[i + 1][v] - rows[i][v] for v in variables] for i in range(count - 1)]
    halves = [None] + [
        [half_minmod(jumps[i - 1][v], jumps[i][v]) for v in variables] for i in range(1, count - 1)
    ]
    fluxes = [None] + [
        twice_flux(
            [rows[i][v] + halves[i][v] for v in variables],
            [rows[i + 1][v] - halves[i + 1][v] for v in variables],
            1,
        )
        for i in range(1, count - 2)
    ]
    result = []
    for i in range(2, count - 2):
        left, right = [], []
        for v in variables:
            q = rows[i][v]
            jump = pltpu.roll(q, 127, 1) - q
            half = half_minmod(pltpu.roll(jump, 1, 1), jump)
            left.append(q + half)
            right.append(pltpu.roll(q - half, 127, 1))
        flux = twice_flux(left, right, 0)
        result.append(
            [
                rows[i][v]
                - (0.5 * COURANT)
                * ((fluxes[i][v] - fluxes[i - 1][v]) + (flux[v] - pltpu.roll(flux[v], 1, 1)))
                for v in variables
            ]
        )
    return result


def turned(x, groups):
    shift = (16 * groups) % 128
    return pltpu.roll(x, shift, 1) if shift else x


def lanes_of(shape):
    return lax.broadcasted_iota(jnp.int32, shape, 1)


def ordered(band_ref, near, far):
    even = jnp.full(near.shape, (band_ref[0] & 1) == 0)
    return jnp.where(even, far, near), jnp.where(even, near, far)


def background_kernel(bands, band_ref, centre_ref, near_ref, far_ref, out_ref):
    low, centre, high = [], [], []
    for r in range(4):
        at = [slice((v * 4 + r) * 8, (v * 4 + r) * 8 + 8) for v in range(5)]
        pairs = [ordered(band_ref, near_ref[x, :], far_ref[x, :]) for x in at]
        low.append([below for below, _ in pairs])
        centre.append([centre_ref[x, :] for x in at])
        high.append([above for _, above in pairs])
    rows = low + centre + high
    rows = transport(rows)
    keep_low = (band_ref[0] > 0).astype(jnp.float32)
    keep_high = (band_ref[0] < bands - 1).astype(jnp.float32)
    for i in (0, 1):
        rows[i] = [x * keep_low for x in rows[i]]
    for i in (6, 7):
        rows[i] = [x * keep_high for x in rows[i]]
    rows = transport(rows)
    lane = lanes_of((8, 128))
    group = lane >> 4
    for q in range(8):
        j = q % 4
        chosen = (q // 4, 2 + q // 4)
        for b in (0, 1):
            slab = None
            for g in range(8):
                u, v = g // 4, g % 4
                piece = turned(rows[chosen[b]][v], g - (2 * j + u))
                slab = piece if slab is None else jnp.where(group == g, piece, slab)
            out_ref[q * 20 + 8 * b : q * 20 + 8 * b + 8, :] = slab
        last = jnp.where(
            lane < 32, turned(rows[chosen[0]][4], -2 * j), turned(rows[chosen[1]][4], 2 - 2 * j)
        )
        out_ref[q * 20 + 16 : q * 20 + 20, :] = jnp.where(
            lane[:4] < 64, last[:4], pltpu.roll(last, 64, 1)[4:]
        )


def statistics_kernel(count_ref, loc_ref, near_ref, value_ref, site_ref, precision_ref, out_ref):
    slot = lanes_of((1, 128))
    sub = lax.broadcasted_iota(jnp.int32, (8, 128), 0)
    lane = lanes_of((8, 128))
    cell = lax.broadcasted_iota(jnp.int32, (128, 128), 0)
    slab = jnp.zeros((8, 128), jnp.float32)
    last = jnp.zeros((8, 128), jnp.float32)
    for u in (0, 1):
        weight = jnp.where(slot < count_ref[u], precision_ref[u : u + 1, :], 0.0)
        both = jnp.where(sub == 0, weight, jnp.where(sub == 1, weight * value_ref[u : u + 1, :], 0.0))
        site = site_ref[u : u + 1, :]
        in_slab = ((cell & 63) == site) & ((cell >> 6) == u)
        in_last = ((64 + (cell & 15)) == site) & (((cell >> 4) & 1) == u)
        dims = (((1,), (1,)), ((), ()))
        slab += lax.dot_general(
            both, in_slab.astype(jnp.float32), dims, precision=HIGHEST,
            preferred_element_type=jnp.float32,
        )
        last += lax.dot_general(
            both, in_last.astype(jnp.float32), dims, precision=HIGHEST,
            preferred_element_type=jnp.float32,
        )
    out = jnp.where(sub < 2, slab, jnp.where(sub < 4, pltpu.roll(last, 2, 0), 0.0))
    for t in (0, 1):
        gain = []
        for u in (0, 1):
            total = jnp.float32(0.0)
            for n in range(3):
                total += jnp.where(near_ref[t, n] == u, loc_ref[t, n], 0.0)
            gain.append(total)
        out = jnp.where(sub == 4 + t, jnp.where((lane >> 6) == 0, gain[0], gain[1]), out)
        out = jnp.where(sub == 6 + t, jnp.where(((lane >> 4) & 1) == 0, gain[0], gain[1]), out)
    out_ref[...] = out


def split(x):
    head = x.astype(jnp.bfloat16)
    return head, (x - head.astype(jnp.float32)).astype(jnp.bfloat16)


def product(left, right, axis):
    return lax.dot_general(
        jnp.concatenate([left[0], left[1], left[0]], axis=1),
        jnp.concatenate([right[0], right[0], right[1]], axis=axis),
        (((1,), (axis,)), ((), ())),
        preferred_element_type=jnp.float32,
    )


def analysis_kernel(half_ref, own_ref, other_ref, own_stats_ref, other_stats_ref, out_ref):
    lane8 = lanes_of((8, 128))
    sub8 = lax.broadcasted_iota(jnp.int32, (8, 128), 0)
    lane = lanes_of((MEMBERS, 128))
    lane1 = lanes_of((1, 128))
    slabs = []
    for b in (0, 1):
        slabs.append(
            jnp.concatenate(
                [
                    ref[s * 20 + 8 * b : s * 20 + 8 * b + 8, :]
                    for ref in (own_ref, other_ref)
                    for s in range(8)
                ],
                axis=0,
            )
        )
    parts = []
    for ref in (own_ref, other_ref):
        for s in range(8):
            four = ref[s * 20 + 16 : s * 20 + 20, :]
            eight = jnp.concatenate([four, four], axis=0)
            eight = jnp.where(sub8 < 4, eight, pltpu.roll(eight, 64, 1))
            parts.append(jnp.where(lane8 < 64, eight, 0.0))
    slabs.append(jnp.concatenate(parts, axis=0))
    means = [jnp.sum(x, axis=0, keepdims=True) * (1.0 / MEMBERS) for x in slabs]
    slabs = [x - m for x, m in zip(slabs, means)]
    first = half_ref[0] == 0
    own = own_stats_ref[...]
    other = other_stats_ref[...]
    stats = [jnp.where(first, own, other), jnp.where(first, other, own)]
    eye = (lax.broadcasted_iota(jnp.int32, (MEMBERS, 128), 0) == lane).astype(jnp.float32)
    tiles = [(b, t) for b in (0, 1) for t in (0, 1)]
    tops, fields, norms = [], [], []
    for b, t in tiles:
        s = stats[b]
        mine = (lane1 >> 5) == b
        gain = s[4 + t : 5 + t]
        gain_last = jnp.where(mine, s[6 + t : 7 + t], 0.0)
        pull = gain * (s[1:2] - s[0:1] * means[b])
        pull_last = gain_last * (s[3:4] - s[2:3] * means[2])
        p, r = slabs[b], slabs[2]
        gram = product(
            split(jnp.concatenate([p * (gain * s[0:1]), r * (gain_last * s[2:3])], axis=1)),
            split(jnp.concatenate([p, r], axis=1)),
            1,
        )
        gram = gram + (MEMBERS - 1.0) * eye
        norm = jnp.sqrt(jnp.sum(jnp.sum(gram * gram, axis=0, keepdims=True), axis=1, keepdims=True))
        norms.append(norm)
        tops.append(gram * (1.0 / norm))
        b_col = jnp.sum(p * pull + r * pull_last, axis=1, keepdims=True)
        if t == 0:
            field = jnp.where(
                lane < 64, p, jnp.where((lane >> 4) == 4 + 2 * b, pltpu.roll(r, 64, 1), 0.0)
            )
            field = jnp.where(lane == 127, b_col, field)
        else:
            field = jnp.where(lane >= 64, p, jnp.where((lane >> 4) == 2 * b + 1, r, 0.0))
            field = jnp.where(lane == 0, b_col, field)
        fields.append(field)
    for sweep in range(NSI):
        factors = [split(1.5 * eye - 0.5 * x) for x in tops]
        if sweep < NSI - 1:
            both = [
                product(f, split(jnp.concatenate([x, y], axis=1)), 0)
                for f, x, y in zip(factors, tops, fields)
            ]
            fields = [x[:, 128:] for x in both]
            tops = [product(split(x[:, :128]), f, 0) for f, x in zip(factors, both)]
        else:
            fields = [product(f, split(y), 0) for f, y in zip(factors, fields)]
    moved = []
    for (b, t), field, norm in zip(tiles, fields, norms):
        column = field[:, 127:128] if t == 0 else field[:, 0:1]
        shift = jnp.sum(column * field, axis=0, keepdims=True) * (1.0 / norm)
        moved.append(field[:64] * jnp.sqrt((MEMBERS - 1.0) / norm) + shift)
    lane64 = lanes_of((64, 128))
    outs = [
        jnp.where(lane64 < 64, moved[0], moved[1]) + means[0],
        jnp.where(lane64 < 64, moved[2], moved[3]) + means[1],
    ]
    group = lane64 >> 4
    last = jnp.where(group == 1, moved[1], pltpu.roll(moved[0], 64, 1))
    last = jnp.where(group == 2, pltpu.roll(moved[2], 64, 1), last)
    last = jnp.where(group == 3, moved[3], last) + means[2]
    for d in range(8):
        for b in (0, 1):
            out_ref[d * 20 + 8 * b : d * 20 + 8 * b + 8, :] = outs[b][8 * d : 8 * d + 8]
        piece = last[8 * d : 8 * d + 8]
        out_ref[d * 20 + 16 : d * 20 + 20, :] = jnp.where(
            lane8[:4] < 64, piece[:4], pltpu.roll(piece, 64, 1)[4:]
        )


def unpack_kernel(band_ref, in_ref, near_ref, far_ref):
    lane = lanes_of((8, 128))
    sub = lax.broadcasted_iota(jnp.int32, (8, 128), 0)
    group = lane >> 4
    lasts = []
    for q in range(8):
        four = in_ref[q * 20 + 16 : q * 20 + 20, :]
        eight = jnp.concatenate([four, four], axis=0)
        lasts.append(jnp.where(sub < 4, eight, pltpu.roll(eight, 64, 1)))
    def field(r, v):
        b, result = r // 2, None
        for j in range(4):
            q = (r % 2) * 4 + j
            if v < 4:
                slab = in_ref[q * 20 + 8 * b : q * 20 + 8 * b + 8, :]
                for u in (0, 1):
                    piece = turned(slab, 2 * j + u - 4 * u - v)
                    result = piece if result is None else jnp.where(group == 2 * j + u, piece, result)
            else:
                piece = turned(lasts[q], 2 * j - 2 * b)
                result = piece if result is None else jnp.where((group >> 1) == j, piece, result)
        return result

    for v in range(5):
        for r in (0, 1):
            at = (v * 2 + r) * 8
            far, near = ordered(band_ref, field(2 + r, v), field(r, v))
            near_ref[at : at + 8, :] = near
            far_ref[at : at + 8, :] = far


def forecast_kernel(band_ref, near_ref, far_ref, from_near_ref, from_far_ref, out_ref):
    below, low, high, above = [], [], [], []
    for r in (0, 1):
        at = [slice((v * 2 + r) * 8, (v * 2 + r) * 8 + 8) for v in range(5)]
        own = [ordered(band_ref, near_ref[x, :], far_ref[x, :]) for x in at]
        got = [ordered(band_ref, from_near_ref[x, :], from_far_ref[x, :]) for x in at]
        low.append([x for x, _ in own])
        high.append([x for _, x in own])
        below.append([x for x, _ in got])
        above.append([x for _, x in got])
    rows = below + low + high + above
    rows = transport(rows)
    for r in range(4):
        for v in range(5):
            out_ref[pl.ds(v * 4 + r, 8, stride=20), :] = rows[r][v]


def array(*shape):
    return jax.ShapeDtypeStruct(shape, jnp.float32)


def call(kernel, in_specs, *out):
    return pl.pallas_call(
        kernel,
        out_shape=out if len(out) > 1 else out[0],
        in_specs=in_specs,
        out_specs=(VMEM,) * len(out) if len(out) > 1 else VMEM,
        compiler_params=SMALL,
    )


def swap(x, axis, first):
    pairs = [(i, i + 1) for i in range(first, lax.axis_size(axis) - 1, 2)]
    return lax.ppermute(x, axis, pairs + [(b, a) for a, b in pairs])


def exchange(x):
    return lax.all_to_all(
        x.reshape(8, 5, 4, 128), "q", split_axis=0, concat_axis=0, tiled=True
    ).reshape(160, 128)


def shards(ensemble, obs_value, obs_site, obs_count, obs_precision, loc_weight, neighbours):
    band = jnp.reshape(lax.axis_index("band"), (1,))
    half = jnp.reshape(lax.axis_index("half"), (1,))
    fields = ensemble.transpose(1, 2, 0, 3).reshape(160, 128)
    near = swap(fields, "band", 0)
    far = swap(fields, "band", 1)
    stats = call(statistics_kernel, [SMEM] * 3 + [VMEM] * 3, array(8, 128))(
        obs_count, loc_weight, neighbours, obs_value, obs_site, obs_precision
    )
    packed = call(
        functools.partial(background_kernel, lax.axis_size("band")),
        [SMEM] + [VMEM] * 3, array(160, 128),
    )(band, fields, near, far)
    own = exchange(packed)
    other = swap(own, "half", 0)
    other_stats = swap(stats, "half", 0)
    analysed = call(analysis_kernel, [SMEM] + [VMEM] * 4, array(160, 128))(
        half, own, other, stats, other_stats
    )
    near, far = call(
        unpack_kernel, [SMEM, VMEM], array(80, 128), array(80, 128)
    )(band, exchange(analysed))
    from_near = swap(near, "band", 0)
    from_far = swap(far, "band", 1)
    out = call(forecast_kernel, [SMEM] + [VMEM] * 4, array(160, 128))(
        band, near, far, from_near, from_far
    )
    return out.reshape(8, 5, 4, 128)


def solution(mesh):
    bands = mesh.shape["band"]
    fine = Mesh(mesh.devices.reshape(bands, 2, 8), ("band", "half", "q"))
    members = ("half", "q")
    tiles = ("band", "half", "q")
    return jax.shard_map(
        shards,
        mesh=fine,
        in_specs=(
            P(members, None, "band", None),
            P(tiles, None),
            P(tiles, None),
            P(tiles),
            P(tiles, None),
            P(tiles, None),
            P(tiles, None),
        ),
        out_specs=P(members, None, "band", None),
        check_vma=False,
    )
```

```python
import functools

import jax
import jax.numpy as jnp
from jax import lax
from jax.experimental import pallas as pl
from jax.experimental.pallas import tpu as pltpu
from jax.sharding import Mesh, PartitionSpec as P

NSI = 6
COURANT = 0.08
HIGHEST = lax.Precision.HIGHEST
MEMBERS = 128
VMEM = pl.BlockSpec(memory_space=pltpu.VMEM)
SMEM = pl.BlockSpec(memory_space=pltpu.SMEM)
SMALL = pltpu.CompilerParams(vmem_limit_bytes=8 * 2**20)


def half_minmod(lower, upper):
    return 0.5 * (
        jnp.maximum(0.0, jnp.minimum(lower, upper)) + jnp.minimum(0.0, jnp.maximum(lower, upper))
    )


def twice_flux(left, right, carrier):
    speed = jnp.maximum(jnp.abs(left[carrier]), jnp.abs(right[carrier]))
    gain_left = left[carrier] + speed
    gain_right = right[carrier] - speed
    return [gain_left * l + gain_right * r for l, r in zip(left, right)]


def transport(rows):
    count, variables = len(rows), range(len(rows[0]))
    jumps = [[rows[i + 1][v] - rows[i][v] for v in variables] for i in range(count - 1)]
    halves = [None] + [
        [half_minmod(jumps[i - 1][v], jumps[i][v]) for v in variables] for i in range(1, count - 1)
    ]
    fluxes = [None] + [
        twice_flux(
            [rows[i][v] + halves[i][v] for v in variables],
            [rows[i + 1][v] - halves[i + 1][v] for v in variables],
            1,
        )
        for i in range(1, count - 2)
    ]
    result = []
    for i in range(2, count - 2):
        left, right = [], []
        for v in variables:
            q = rows[i][v]
            jump = pltpu.roll(q, 127, 1) - q
            half = half_minmod(pltpu.roll(jump, 1, 1), jump)
            left.append(q + half)
            right.append(pltpu.roll(q - half, 127, 1))
        flux = twice_flux(left, right, 0)
        result.append(
            [
                rows[i][v]
                - (0.5 * COURANT)
                * ((fluxes[i][v] - fluxes[i - 1][v]) + (flux[v] - pltpu.roll(flux[v], 1, 1)))
                for v in variables
            ]
        )
    return result


def turned(x, groups):
    shift = (16 * groups) % 128
    return pltpu.roll(x, shift, 1) if shift else x


def lanes_of(shape):
    return lax.broadcasted_iota(jnp.int32, shape, 1)


def ordered(band_ref, near, far):
    even = jnp.full(near.shape, (band_ref[0] & 1) == 0)
    return jnp.where(even, far, near), jnp.where(even, near, far)


def background_kernel(bands, band_ref, centre_ref, near_ref, far_ref, out_ref):
    low, centre, high = [], [], []
    for r in range(4):
        at = [slice((v * 4 + r) * 8, (v * 4 + r) * 8 + 8) for v in range(5)]
        pairs = [ordered(band_ref, near_ref[x, :], far_ref[x, :]) for x in at]
        low.append([below for below, _ in pairs])
        centre.append([centre_ref[x, :] for x in at])
        high.append([above for _, above in pairs])
    rows = low + centre + high
    rows = transport(rows)
    keep_low = (band_ref[0] > 0).astype(jnp.float32)
    keep_high = (band_ref[0] < bands - 1).astype(jnp.float32)
    for i in (0, 1):
        rows[i] = [x * keep_low for x in rows[i]]
    for i in (6, 7):
        rows[i] = [x * keep_high for x in rows[i]]
    rows = transport(rows)
    lane = lanes_of((8, 128))
    group = lane >> 4
    for q in range(8):
        j = q % 4
        chosen = (q // 4, 2 + q // 4)
        for b in (0, 1):
            slab = None
            for g in range(8):
                u, v = g // 4, g % 4
                piece = turned(rows[chosen[b]][v], g - (2 * j + u))
                slab = piece if slab is None else jnp.where(group == g, piece, slab)
            out_ref[q * 20 + 8 * b : q * 20 + 8 * b + 8, :] = slab
        last = jnp.where(
            lane < 32, turned(rows[chosen[0]][4], -2 * j), turned(rows[chosen[1]][4], 2 - 2 * j)
        )
        out_ref[q * 20 + 16 : q * 20 + 20, :] = jnp.where(
            lane[:4] < 64, last[:4], pltpu.roll(last, 64, 1)[4:]
        )


def statistics_kernel(count_ref, loc_ref, near_ref, value_ref, site_ref, precision_ref, out_ref):
    slot = lanes_of((1, 128))
    sub = lax.broadcasted_iota(jnp.int32, (8, 128), 0)
    lane = lanes_of((8, 128))
    cell = lax.broadcasted_iota(jnp.int32, (128, 128), 0)
    slab = jnp.zeros((8, 128), jnp.float32)
    last = jnp.zeros((8, 128), jnp.float32)
    for u in (0, 1):
        weight = jnp.where(slot < count_ref[u], precision_ref[u : u + 1, :], 0.0)
        both = jnp.where(sub == 0, weight, jnp.where(sub == 1, weight * value_ref[u : u + 1, :], 0.0))
        site = site_ref[u : u + 1, :]
        in_slab = ((cell & 63) == site) & ((cell >> 6) == u)
        in_last = ((64 + (cell & 15)) == site) & (((cell >> 4) & 1) == u)
        dims = (((1,), (1,)), ((), ()))
        slab += lax.dot_general(
            both, in_slab.astype(jnp.float32), dims, precision=HIGHEST,
            preferred_element_type=jnp.float32,
        )
        last += lax.dot_general(
            both, in_last.astype(jnp.float32), dims, precision=HIGHEST,
            preferred_element_type=jnp.float32,
        )
    out = jnp.where(sub < 2, slab, jnp.where(sub < 4, pltpu.roll(last, 2, 0), 0.0))
    for t in (0, 1):
        gain = []
        for u in (0, 1):
            total = jnp.float32(0.0)
            for n in range(3):
                total += jnp.where(near_ref[t, n] == u, loc_ref[t, n], 0.0)
            gain.append(total)
        out = jnp.where(sub == 4 + t, jnp.where((lane >> 6) == 0, gain[0], gain[1]), out)
        out = jnp.where(sub == 6 + t, jnp.where(((lane >> 4) & 1) == 0, gain[0], gain[1]), out)
    out_ref[...] = out


def split(x):
    head = x.astype(jnp.bfloat16)
    return head, (x - head.astype(jnp.float32)).astype(jnp.bfloat16)


def product(left, right, axis):
    return lax.dot_general(
        jnp.concatenate([left[0], left[1], left[0]], axis=1),
        jnp.concatenate([right[0], right[0], right[1]], axis=axis),
        (((1,), (axis,)), ((), ())),
        preferred_element_type=jnp.float32,
    )


def analysis_kernel(half_ref, own_ref, other_ref, own_stats_ref, out_ref):
    lane8 = lanes_of((8, 128))
    sub8 = lax.broadcasted_iota(jnp.int32, (8, 128), 0)
    lane = lanes_of((MEMBERS, 128))
    lane1 = lanes_of((1, 128))
    slabs = []
    for b in (0, 1):
        slabs.append(
            jnp.concatenate(
                [
                    ref[s * 20 + 8 * b : s * 20 + 8 * b + 8, :]
                    for ref in (own_ref, other_ref)
                    for s in range(8)
                ],
                axis=0,
            )
        )
    parts = []
    for ref in (own_ref, other_ref):
        for s in range(8):
            four = ref[s * 20 + 16 : s * 20 + 20, :]
            eight = jnp.concatenate([four, four], axis=0)
            eight = jnp.where(sub8 < 4, eight, pltpu.roll(eight, 64, 1))
            parts.append(jnp.where(lane8 < 64, eight, 0.0))
    slabs.append(jnp.concatenate(parts, axis=0))
    means = [jnp.sum(x, axis=0, keepdims=True) * (1.0 / MEMBERS) for x in slabs]
    slabs = [x - m for x, m in zip(slabs, means)]
    first = half_ref[0] == 0
    own = own_stats_ref[...]
    other = other_ref[160:168, :]
    stats = [jnp.where(first, own, other), jnp.where(first, other, own)]
    eye = (lax.broadcasted_iota(jnp.int32, (MEMBERS, 128), 0) == lane).astype(jnp.float32)
    tiles = [(b, t) for b in (0, 1) for t in (0, 1)]
    tops, fields, norms = [], [], []
    for b, t in tiles:
        s = stats[b]
        mine = (lane1 >> 5) == b
        gain = s[4 + t : 5 + t]
        gain_last = jnp.where(mine, s[6 + t : 7 + t], 0.0)
        pull = gain * (s[1:2] - s[0:1] * means[b])
        pull_last = gain_last * (s[3:4] - s[2:3] * means[2])
        p, r = slabs[b], slabs[2]
        gram = product(
            split(jnp.concatenate([p * (gain * s[0:1]), r * (gain_last * s[2:3])], axis=1)),
            split(jnp.concatenate([p, r], axis=1)),
            1,
        )
        gram = gram + (MEMBERS - 1.0) * eye
        norm = jnp.sqrt(jnp.sum(jnp.sum(gram * gram, axis=0, keepdims=True), axis=1, keepdims=True))
        norms.append(norm)
        tops.append(gram * (1.0 / norm))
        b_col = jnp.sum(p * pull + r * pull_last, axis=1, keepdims=True)
        if t == 0:
            field = jnp.where(
                lane < 64, p, jnp.where((lane >> 4) == 4 + 2 * b, pltpu.roll(r, 64, 1), 0.0)
            )
            field = jnp.where(lane == 127, b_col, field)
        else:
            field = jnp.where(lane >= 64, p, jnp.where((lane >> 4) == 2 * b + 1, r, 0.0))
            field = jnp.where(lane == 0, b_col, field)
        fields.append(field)
    for sweep in range(NSI):
        factors = [split(1.5 * eye - 0.5 * x) for x in tops]
        if sweep < NSI - 1:
            both = [
                product(f, split(jnp.concatenate([x, y], axis=1)), 0)
                for f, x, y in zip(factors, tops, fields)
            ]
            fields = [x[:, 128:] for x in both]
            tops = [product(split(x[:, :128]), f, 0) for f, x in zip(factors, both)]
        else:
            fields = [product(f, split(y), 0) for f, y in zip(factors, fields)]
    moved = []
    for (b, t), field, norm in zip(tiles, fields, norms):
        column = field[:, 127:128] if t == 0 else field[:, 0:1]
        shift = jnp.sum(column * field, axis=0, keepdims=True) * (1.0 / norm)
        moved.append(field[:64] * jnp.sqrt((MEMBERS - 1.0) / norm) + shift)
    lane64 = lanes_of((64, 128))
    outs = [
        jnp.where(lane64 < 64, moved[0], moved[1]) + means[0],
        jnp.where(lane64 < 64, moved[2], moved[3]) + means[1],
    ]
    group = lane64 >> 4
    last = jnp.where(group == 1, moved[1], pltpu.roll(moved[0], 64, 1))
    last = jnp.where(group == 2, pltpu.roll(moved[2], 64, 1), last)
    last = jnp.where(group == 3, moved[3], last) + means[2]
    for d in range(8):
        for b in (0, 1):
            out_ref[d * 20 + 8 * b : d * 20 + 8 * b + 8, :] = outs[b][8 * d : 8 * d + 8]
        piece = last[8 * d : 8 * d + 8]
        out_ref[d * 20 + 16 : d * 20 + 20, :] = jnp.where(
            lane8[:4] < 64, piece[:4], pltpu.roll(piece, 64, 1)[4:]
        )


def unpack_kernel(band_ref, in_ref, near_ref, far_ref):
    lane = lanes_of((8, 128))
    sub = lax.broadcasted_iota(jnp.int32, (8, 128), 0)
    group = lane >> 4
    lasts = []
    for q in range(8):
        four = in_ref[q * 20 + 16 : q * 20 + 20, :]
        eight = jnp.concatenate([four, four], axis=0)
        lasts.append(jnp.where(sub < 4, eight, pltpu.roll(eight, 64, 1)))
    def field(r, v):
        b, result = r // 2, None
        for j in range(4):
            q = (r % 2) * 4 + j
            if v < 4:
                slab = in_ref[q * 20 + 8 * b : q * 20 + 8 * b + 8, :]
                for u in (0, 1):
                    piece = turned(slab, 2 * j + u - 4 * u - v)
                    result = piece if result is None else jnp.where(group == 2 * j + u, piece, result)
            else:
                piece = turned(lasts[q], 2 * j - 2 * b)
                result = piece if result is None else jnp.where((group >> 1) == j, piece, result)
        return result

    for v in range(5):
        for r in (0, 1):
            at = (v * 2 + r) * 8
            far, near = ordered(band_ref, field(2 + r, v), field(r, v))
            near_ref[at : at + 8, :] = near
            far_ref[at : at + 8, :] = far


def forecast_kernel(band_ref, near_ref, far_ref, from_near_ref, from_far_ref, out_ref):
    below, low, high, above = [], [], [], []
    for r in (0, 1):
        at = [slice((v * 2 + r) * 8, (v * 2 + r) * 8 + 8) for v in range(5)]
        own = [ordered(band_ref, near_ref[x, :], far_ref[x, :]) for x in at]
        got = [ordered(band_ref, from_near_ref[x, :], from_far_ref[x, :]) for x in at]
        low.append([x for x, _ in own])
        high.append([x for _, x in own])
        below.append([x for x, _ in got])
        above.append([x for _, x in got])
    rows = below + low + high + above
    rows = transport(rows)
    for r in range(4):
        for v in range(5):
            out_ref[pl.ds(v * 4 + r, 8, stride=20), :] = rows[r][v]


def array(*shape):
    return jax.ShapeDtypeStruct(shape, jnp.float32)


def call(kernel, in_specs, *out):
    return pl.pallas_call(
        kernel,
        out_shape=out if len(out) > 1 else out[0],
        in_specs=in_specs,
        out_specs=(VMEM,) * len(out) if len(out) > 1 else VMEM,
        compiler_params=SMALL,
    )


def swap(x, axis, first):
    pairs = [(i, i + 1) for i in range(first, lax.axis_size(axis) - 1, 2)]
    return lax.ppermute(x, axis, pairs + [(b, a) for a, b in pairs])


def exchange(x):
    return lax.all_to_all(
        x.reshape(8, 5, 4, 128), "q", split_axis=0, concat_axis=0, tiled=True
    ).reshape(160, 128)


def shards(ensemble, obs_value, obs_site, obs_count, obs_precision, loc_weight, neighbours):
    band = jnp.reshape(lax.axis_index("band"), (1,))
    half = jnp.reshape(lax.axis_index("half"), (1,))
    fields = ensemble.transpose(1, 2, 0, 3).reshape(160, 128)
    near = swap(fields, "band", 0)
    far = swap(fields, "band", 1)
    stats = call(statistics_kernel, [SMEM] * 3 + [VMEM] * 3, array(8, 128))(
        obs_count, loc_weight, neighbours, obs_value, obs_site, obs_precision
    )
    packed = call(
        functools.partial(background_kernel, lax.axis_size("band")),
        [SMEM] + [VMEM] * 3, array(160, 128),
    )(band, fields, near, far)
    own = exchange(packed)
    other = swap(jnp.concatenate([own, stats], axis=0), "half", 0)
    analysed = call(analysis_kernel, [SMEM] + [VMEM] * 3, array(160, 128))(half, own, other, stats)
    near, far = call(
        unpack_kernel, [SMEM, VMEM], array(80, 128), array(80, 128)
    )(band, exchange(analysed))
    from_near = swap(near, "band", 0)
    from_far = swap(far, "band", 1)
    out = call(forecast_kernel, [SMEM] + [VMEM] * 4, array(160, 128))(
        band, near, far, from_near, from_far
    )
    return out.reshape(8, 5, 4, 128)


def solution(mesh):
    bands = mesh.shape["band"]
    fine = Mesh(mesh.devices.reshape(bands, 2, 8), ("band", "half", "q"))
    members = ("half", "q")
    tiles = ("band", "half", "q")
    return jax.shard_map(
        shards,
        mesh=fine,
        in_specs=(
            P(members, None, "band", None),
            P(tiles, None),
            P(tiles, None),
            P(tiles),
            P(tiles, None),
            P(tiles, None),
            P(tiles, None),
        ),
        out_specs=P(members, None, "band", None),
        check_vma=False,
    )
```

```python
import functools

import jax
import jax.numpy as jnp
from jax import lax
from jax.experimental import pallas as pl
from jax.experimental.pallas import tpu as pltpu
from jax.sharding import Mesh, PartitionSpec as P

NSI = 6
COURANT = 0.08
HIGHEST = lax.Precision.HIGHEST
MEMBERS = 128
VMEM = pl.BlockSpec(memory_space=pltpu.VMEM)
SMEM = pl.BlockSpec(memory_space=pltpu.SMEM)
SMALL = pltpu.CompilerParams(vmem_limit_bytes=8 * 2**20)


def half_minmod(lower, upper):
    return 0.5 * (
        jnp.maximum(0.0, jnp.minimum(lower, upper)) + jnp.minimum(0.0, jnp.maximum(lower, upper))
    )


def twice_flux(left, right, carrier):
    speed = jnp.maximum(jnp.abs(left[carrier]), jnp.abs(right[carrier]))
    gain_left = left[carrier] + speed
    gain_right = right[carrier] - speed
    return [gain_left * l + gain_right * r for l, r in zip(left, right)]


def transport(rows):
    count, variables = len(rows), range(len(rows[0]))
    jumps = [[rows[i + 1][v] - rows[i][v] for v in variables] for i in range(count - 1)]
    halves = [None] + [
        [half_minmod(jumps[i - 1][v], jumps[i][v]) for v in variables] for i in range(1, count - 1)
    ]
    fluxes = [None] + [
        twice_flux(
            [rows[i][v] + halves[i][v] for v in variables],
            [rows[i + 1][v] - halves[i + 1][v] for v in variables],
            1,
        )
        for i in range(1, count - 2)
    ]
    result = []
    for i in range(2, count - 2):
        left, right = [], []
        for v in variables:
            q = rows[i][v]
            jump = pltpu.roll(q, 127, 1) - q
            half = half_minmod(pltpu.roll(jump, 1, 1), jump)
            left.append(q + half)
            right.append(pltpu.roll(q - half, 127, 1))
        flux = twice_flux(left, right, 0)
        result.append(
            [
                rows[i][v]
                - (0.5 * COURANT)
                * ((fluxes[i][v] - fluxes[i - 1][v]) + (flux[v] - pltpu.roll(flux[v], 1, 1)))
                for v in variables
            ]
        )
    return result


def turned(x, groups):
    shift = (16 * groups) % 128
    return pltpu.roll(x, shift, 1) if shift else x


def lanes_of(shape):
    return lax.broadcasted_iota(jnp.int32, shape, 1)


def ordered(band_ref, near, far):
    even = jnp.full(near.shape, (band_ref[0] & 1) == 0)
    return jnp.where(even, far, near), jnp.where(even, near, far)


def background_kernel(bands, band_ref, centre_ref, near_ref, far_ref, out_ref):
    low, centre, high = [], [], []
    for r in range(4):
        at = [slice((v * 4 + r) * 8, (v * 4 + r) * 8 + 8) for v in range(5)]
        pairs = [ordered(band_ref, near_ref[x, :], far_ref[x, :]) for x in at]
        low.append([below for below, _ in pairs])
        centre.append([centre_ref[x, :] for x in at])
        high.append([above for _, above in pairs])
    rows = low + centre + high
    rows = transport(rows)
    keep_low = (band_ref[0] > 0).astype(jnp.float32)
    keep_high = (band_ref[0] < bands - 1).astype(jnp.float32)
    for i in (0, 1):
        rows[i] = [x * keep_low for x in rows[i]]
    for i in (6, 7):
        rows[i] = [x * keep_high for x in rows[i]]
    rows = transport(rows)
    lane = lanes_of((8, 128))
    group = lane >> 4
    for q in range(8):
        j = q % 4
        chosen = (q // 4, 2 + q // 4)
        for b in (0, 1):
            slab = None
            for g in range(8):
                u, v = g // 4, g % 4
                piece = turned(rows[chosen[b]][v], g - (2 * j + u))
                slab = piece if slab is None else jnp.where(group == g, piece, slab)
            out_ref[q * 20 + 8 * b : q * 20 + 8 * b + 8, :] = slab
        last = jnp.where(
            lane < 32, turned(rows[chosen[0]][4], -2 * j), turned(rows[chosen[1]][4], 2 - 2 * j)
        )
        out_ref[q * 20 + 16 : q * 20 + 20, :] = jnp.where(
            lane[:4] < 64, last[:4], pltpu.roll(last, 64, 1)[4:]
        )


def statistics_kernel(count_ref, loc_ref, near_ref, value_ref, site_ref, precision_ref, out_ref):
    slot = lanes_of((1, 128))
    sub = lax.broadcasted_iota(jnp.int32, (8, 128), 0)
    lane = lanes_of((8, 128))
    cell = lax.broadcasted_iota(jnp.int32, (128, 128), 0)
    slab = jnp.zeros((8, 128), jnp.float32)
    last = jnp.zeros((8, 128), jnp.float32)
    for u in (0, 1):
        weight = jnp.where(slot < count_ref[u], precision_ref[u : u + 1, :], 0.0)
        both = jnp.where(sub == 0, weight, jnp.where(sub == 1, weight * value_ref[u : u + 1, :], 0.0))
        site = site_ref[u : u + 1, :]
        in_slab = ((cell & 63) == site) & ((cell >> 6) == u)
        in_last = ((64 + (cell & 15)) == site) & (((cell >> 4) & 1) == u)
        dims = (((1,), (1,)), ((), ()))
        slab += lax.dot_general(
            both, in_slab.astype(jnp.float32), dims, precision=HIGHEST,
            preferred_element_type=jnp.float32,
        )
        last += lax.dot_general(
            both, in_last.astype(jnp.float32), dims, precision=HIGHEST,
            preferred_element_type=jnp.float32,
        )
    out = jnp.where(sub < 2, slab, jnp.where(sub < 4, pltpu.roll(last, 2, 0), 0.0))
    for t in (0, 1):
        gain = []
        for u in (0, 1):
            total = jnp.float32(0.0)
            for n in range(3):
                total += jnp.where(near_ref[t, n] == u, loc_ref[t, n], 0.0)
            gain.append(total)
        out = jnp.where(sub == 4 + t, jnp.where((lane >> 6) == 0, gain[0], gain[1]), out)
        out = jnp.where(sub == 6 + t, jnp.where(((lane >> 4) & 1) == 0, gain[0], gain[1]), out)
    out_ref[...] = out


def split(x):
    head = x.astype(jnp.bfloat16)
    return head, (x - head.astype(jnp.float32)).astype(jnp.bfloat16)


def product(left, right, axis):
    return lax.dot_general(
        jnp.concatenate([left[0], left[1], left[0]], axis=1),
        jnp.concatenate([right[0], right[0], right[1]], axis=axis),
        (((1,), (axis,)), ((), ())),
        preferred_element_type=jnp.float32,
    )


def first_analysis_kernel(half_ref, own_ref, other_ref, own_stats_ref, out_ref):
    @pl.when(half_ref[0] == 0)
    def _():
        analysis(half_ref, own_ref, other_ref, own_stats_ref, out_ref)


def second_analysis_kernel(half_ref, own_ref, other_ref, own_stats_ref, first_ref, out_ref):
    @pl.when(half_ref[0] == 0)
    def _():
        out_ref[...] = first_ref[...]

    @pl.when(half_ref[0] == 1)
    def _():
        analysis(half_ref, own_ref, other_ref, own_stats_ref, out_ref)


def analysis(half_ref, own_ref, other_ref, own_stats_ref, out_ref):
    lane8 = lanes_of((8, 128))
    sub8 = lax.broadcasted_iota(jnp.int32, (8, 128), 0)
    lane = lanes_of((MEMBERS, 128))
    lane1 = lanes_of((1, 128))
    slabs = []
    for b in (0, 1):
        slabs.append(
            jnp.concatenate(
                [
                    ref[s * 20 + 8 * b : s * 20 + 8 * b + 8, :]
                    for ref in (own_ref, other_ref)
                    for s in range(8)
                ],
                axis=0,
            )
        )
    parts = []
    for ref in (own_ref, other_ref):
        for s in range(8):
            four = ref[s * 20 + 16 : s * 20 + 20, :]
            eight = jnp.concatenate([four, four], axis=0)
            eight = jnp.where(sub8 < 4, eight, pltpu.roll(eight, 64, 1))
            parts.append(jnp.where(lane8 < 64, eight, 0.0))
    slabs.append(jnp.concatenate(parts, axis=0))
    means = [jnp.sum(x, axis=0, keepdims=True) * (1.0 / MEMBERS) for x in slabs]
    slabs = [x - m for x, m in zip(slabs, means)]
    first = half_ref[0] == 0
    own = own_stats_ref[...]
    other = other_ref[160:168, :]
    stats = [jnp.where(first, own, other), jnp.where(first, other, own)]
    eye = (lax.broadcasted_iota(jnp.int32, (MEMBERS, 128), 0) == lane).astype(jnp.float32)
    tiles = [(b, t) for b in (0, 1) for t in (0, 1)]
    tops, fields, norms = [], [], []
    for b, t in tiles:
        s = stats[b]
        mine = (lane1 >> 5) == b
        gain = s[4 + t : 5 + t]
        gain_last = jnp.where(mine, s[6 + t : 7 + t], 0.0)
        pull = gain * (s[1:2] - s[0:1] * means[b])
        pull_last = gain_last * (s[3:4] - s[2:3] * means[2])
        p, r = slabs[b], slabs[2]
        gram = product(
            split(jnp.concatenate([p * (gain * s[0:1]), r * (gain_last * s[2:3])], axis=1)),
            split(jnp.concatenate([p, r], axis=1)),
            1,
        )
        gram = gram + (MEMBERS - 1.0) * eye
        norm = jnp.sqrt(jnp.sum(jnp.sum(gram * gram, axis=0, keepdims=True), axis=1, keepdims=True))
        norms.append(norm)
        tops.append(gram * (1.0 / norm))
        b_col = jnp.sum(p * pull + r * pull_last, axis=1, keepdims=True)
        if t == 0:
            field = jnp.where(
                lane < 64, p, jnp.where((lane >> 4) == 4 + 2 * b, pltpu.roll(r, 64, 1), 0.0)
            )
            field = jnp.where(lane == 127, b_col, field)
        else:
            field = jnp.where(lane >= 64, p, jnp.where((lane >> 4) == 2 * b + 1, r, 0.0))
            field = jnp.where(lane == 0, b_col, field)
        fields.append(field)
    for sweep in range(NSI):
        factors = [split(1.5 * eye - 0.5 * x) for x in tops]
        if sweep < NSI - 1:
            both = [
                product(f, split(jnp.concatenate([x, y], axis=1)), 0)
                for f, x, y in zip(factors, tops, fields)
            ]
            fields = [x[:, 128:] for x in both]
            tops = [product(split(x[:, :128]), f, 0) for f, x in zip(factors, both)]
        else:
            fields = [product(f, split(y), 0) for f, y in zip(factors, fields)]
    moved = []
    for (b, t), field, norm in zip(tiles, fields, norms):
        column = field[:, 127:128] if t == 0 else field[:, 0:1]
        shift = jnp.sum(column * field, axis=0, keepdims=True) * (1.0 / norm)
        moved.append(field[:64] * jnp.sqrt((MEMBERS - 1.0) / norm) + shift)
    lane64 = lanes_of((64, 128))
    outs = [
        jnp.where(lane64 < 64, moved[0], moved[1]) + means[0],
        jnp.where(lane64 < 64, moved[2], moved[3]) + means[1],
    ]
    group = lane64 >> 4
    last = jnp.where(group == 1, moved[1], pltpu.roll(moved[0], 64, 1))
    last = jnp.where(group == 2, pltpu.roll(moved[2], 64, 1), last)
    last = jnp.where(group == 3, moved[3], last) + means[2]
    for d in range(8):
        for b in (0, 1):
            out_ref[d * 20 + 8 * b : d * 20 + 8 * b + 8, :] = outs[b][8 * d : 8 * d + 8]
        piece = last[8 * d : 8 * d + 8]
        out_ref[d * 20 + 16 : d * 20 + 20, :] = jnp.where(
            lane8[:4] < 64, piece[:4], pltpu.roll(piece, 64, 1)[4:]
        )


def unpack_kernel(band_ref, in_ref, near_ref, far_ref):
    lane = lanes_of((8, 128))
    sub = lax.broadcasted_iota(jnp.int32, (8, 128), 0)
    group = lane >> 4
    lasts = []
    for q in range(8):
        four = in_ref[q * 20 + 16 : q * 20 + 20, :]
        eight = jnp.concatenate([four, four], axis=0)
        lasts.append(jnp.where(sub < 4, eight, pltpu.roll(eight, 64, 1)))

    def field(r, v):
        b, result = r // 2, None
        for j in range(4):
            q = (r % 2) * 4 + j
            if v < 4:
                slab = in_ref[q * 20 + 8 * b : q * 20 + 8 * b + 8, :]
                for u in (0, 1):
                    piece = turned(slab, 2 * j + u - 4 * u - v)
                    result = piece if result is None else jnp.where(group == 2 * j + u, piece, result)
            else:
                piece = turned(lasts[q], 2 * j - 2 * b)
                result = piece if result is None else jnp.where((group >> 1) == j, piece, result)
        return result

    for v in range(5):
        for r in (0, 1):
            at = (v * 2 + r) * 8
            far, near = ordered(band_ref, field(2 + r, v), field(r, v))
            near_ref[at : at + 8, :] = near
            far_ref[at : at + 8, :] = far


def forecast_kernel(band_ref, near_ref, far_ref, from_near_ref, from_far_ref, out_ref):
    below, low, high, above = [], [], [], []
    for r in (0, 1):
        at = [slice((v * 2 + r) * 8, (v * 2 + r) * 8 + 8) for v in range(5)]
        own = [ordered(band_ref, near_ref[x, :], far_ref[x, :]) for x in at]
        got = [ordered(band_ref, from_near_ref[x, :], from_far_ref[x, :]) for x in at]
        low.append([x for x, _ in own])
        high.append([x for _, x in own])
        below.append([x for x, _ in got])
        above.append([x for _, x in got])
    rows = below + low + high + above
    rows = transport(rows)
    for r in range(4):
        for v in range(5):
            out_ref[pl.ds(v * 4 + r, 8, stride=20), :] = rows[r][v]


def array(*shape):
    return jax.ShapeDtypeStruct(shape, jnp.float32)


def call(kernel, in_specs, *out):
    return pl.pallas_call(
        kernel,
        out_shape=out if len(out) > 1 else out[0],
        in_specs=in_specs,
        out_specs=(VMEM,) * len(out) if len(out) > 1 else VMEM,
        compiler_params=SMALL,
    )


def swap(x, axis, first):
    pairs = [(i, i + 1) for i in range(first, lax.axis_size(axis) - 1, 2)]
    return lax.ppermute(x, axis, pairs + [(b, a) for a, b in pairs])


def one_way(x, axis, pair):
    return lax.ppermute(x, axis, [pair])


def exchange(x):
    return lax.all_to_all(
        x.reshape(8, 5, 4, 128), "q", split_axis=0, concat_axis=0, tiled=True
    ).reshape(160, 128)


def shards(ensemble, obs_value, obs_site, obs_count, obs_precision, loc_weight, neighbours):
    band = jnp.reshape(lax.axis_index("band"), (1,))
    half = jnp.reshape(lax.axis_index("half"), (1,))
    fields = ensemble.transpose(1, 2, 0, 3).reshape(160, 128)
    near = swap(fields, "band", 0)
    far = swap(fields, "band", 1)
    stats = call(statistics_kernel, [SMEM] * 3 + [VMEM] * 3, array(8, 128))(
        obs_count, loc_weight, neighbours, obs_value, obs_site, obs_precision
    )
    packed = call(
        functools.partial(background_kernel, lax.axis_size("band")),
        [SMEM] + [VMEM] * 3, array(160, 128),
    )(band, fields, near, far)
    own = exchange(packed)
    crossing = jnp.concatenate([own, stats], axis=0)
    other = one_way(crossing, "half", (1, 0))
    first = call(first_analysis_kernel, [SMEM] + [VMEM] * 3, array(160, 128))(
        half, own, other, stats
    )
    other = one_way(crossing, "half", (0, 1))
    analysed = call(
        second_analysis_kernel, [SMEM] + [VMEM] * 4, array(160, 128)
    )(half, own, other, stats, first)
    near, far = call(
        unpack_kernel, [SMEM, VMEM], array(80, 128), array(80, 128)
    )(band, exchange(analysed))
    from_near = swap(near, "band", 0)
    from_far = swap(far, "band", 1)
    out = call(forecast_kernel, [SMEM] + [VMEM] * 4, array(160, 128))(
        band, near, far, from_near, from_far
    )
    return out.reshape(8, 5, 4, 128)


def solution(mesh):
    bands = mesh.shape["band"]
    fine = Mesh(mesh.devices.reshape(bands, 2, 8), ("band", "half", "q"))
    members = ("half", "q")
    tiles = ("band", "half", "q")
    return jax.shard_map(
        shards,
        mesh=fine,
        in_specs=(
            P(members, None, "band", None),
            P(tiles, None),
            P(tiles, None),
            P(tiles),
            P(tiles, None),
            P(tiles, None),
            P(tiles, None),
        ),
        out_specs=P(members, None, "band", None),
        check_vma=False,
    )
```

```python
import functools

import jax
import jax.numpy as jnp
from jax import lax
from jax.experimental import pallas as pl
from jax.experimental.pallas import tpu as pltpu
from jax.sharding import Mesh, PartitionSpec as P

NSI = 6
COURANT = 0.08
HIGHEST = lax.Precision.HIGHEST
MEMBERS = 128
VMEM = pl.BlockSpec(memory_space=pltpu.VMEM)
SMEM = pl.BlockSpec(memory_space=pltpu.SMEM)
SMALL = pltpu.CompilerParams(vmem_limit_bytes=8 * 2**20)


def half_minmod(lower, upper):
    return 0.5 * (
        jnp.maximum(0.0, jnp.minimum(lower, upper)) + jnp.minimum(0.0, jnp.maximum(lower, upper))
    )


def twice_flux(left, right, carrier):
    speed = jnp.maximum(jnp.abs(left[carrier]), jnp.abs(right[carrier]))
    gain_left = left[carrier] + speed
    gain_right = right[carrier] - speed
    return [gain_left * l + gain_right * r for l, r in zip(left, right)]


def transport(rows):
    count, variables = len(rows), range(len(rows[0]))
    jumps = [[rows[i + 1][v] - rows[i][v] for v in variables] for i in range(count - 1)]
    halves = [None] + [
        [half_minmod(jumps[i - 1][v], jumps[i][v]) for v in variables] for i in range(1, count - 1)
    ]
    fluxes = [None] + [
        twice_flux(
            [rows[i][v] + halves[i][v] for v in variables],
            [rows[i + 1][v] - halves[i + 1][v] for v in variables],
            1,
        )
        for i in range(1, count - 2)
    ]
    result = []
    for i in range(2, count - 2):
        left, right = [], []
        for v in variables:
            q = rows[i][v]
            jump = pltpu.roll(q, 127, 1) - q
            half = half_minmod(pltpu.roll(jump, 1, 1), jump)
            left.append(q + half)
            right.append(pltpu.roll(q - half, 127, 1))
        flux = twice_flux(left, right, 0)
        result.append(
            [
                rows[i][v]
                - (0.5 * COURANT)
                * ((fluxes[i][v] - fluxes[i - 1][v]) + (flux[v] - pltpu.roll(flux[v], 1, 1)))
                for v in variables
            ]
        )
    return result


def turned(x, groups):
    shift = (16 * groups) % 128
    return pltpu.roll(x, shift, 1) if shift else x


def lanes_of(shape):
    return lax.broadcasted_iota(jnp.int32, shape, 1)


def ordered(band_ref, near, far):
    even = jnp.full(near.shape, (band_ref[0] & 1) == 0)
    return jnp.where(even, far, near), jnp.where(even, near, far)


def background_kernel(bands, band_ref, centre_ref, near_ref, far_ref, stats_ref, own_ref, out_ref):
    out_ref[160:168, :] = stats_ref[...]
    low, centre, high = [], [], []
    for r in range(4):
        at = [slice((v * 4 + r) * 8, (v * 4 + r) * 8 + 8) for v in range(5)]
        pairs = [ordered(band_ref, near_ref[x, :], far_ref[x, :]) for x in at]
        low.append([below for below, _ in pairs])
        centre.append([centre_ref[x, :] for x in at])
        high.append([above for _, above in pairs])
    rows = low + centre + high
    rows = transport(rows)
    keep_low = (band_ref[0] > 0).astype(jnp.float32)
    keep_high = (band_ref[0] < bands - 1).astype(jnp.float32)
    for i in (0, 1):
        rows[i] = [x * keep_low for x in rows[i]]
    for i in (6, 7):
        rows[i] = [x * keep_high for x in rows[i]]
    rows = transport(rows)
    lane = lanes_of((8, 128))
    group = lane >> 4
    for q in range(8):
        j = q % 4
        chosen = (q // 4, 2 + q // 4)
        for b in (0, 1):
            slab = None
            for g in range(8):
                u, v = g // 4, g % 4
                piece = turned(rows[chosen[b]][v], g - (2 * j + u))
                slab = piece if slab is None else jnp.where(group == g, piece, slab)
            own_ref[q * 20 + 8 * b : q * 20 + 8 * b + 8, :] = slab
            out_ref[q * 20 + 8 * b : q * 20 + 8 * b + 8, :] = slab
        last = jnp.where(
            lane < 32, turned(rows[chosen[0]][4], -2 * j), turned(rows[chosen[1]][4], 2 - 2 * j)
        )
        four = jnp.where(lane[:4] < 64, last[:4], pltpu.roll(last, 64, 1)[4:])
        own_ref[q * 20 + 16 : q * 20 + 20, :] = four
        out_ref[q * 20 + 16 : q * 20 + 20, :] = four


def strip_kernel(in_ref, own_ref, half_ref, out_ref, stats_ref):
    out_ref[...] = in_ref[:160, :]
    stats_ref[...] = in_ref[160:168, :]


def statistics_kernel(count_ref, loc_ref, near_ref, value_ref, site_ref, precision_ref, out_ref):
    slot = lanes_of((1, 128))
    sub = lax.broadcasted_iota(jnp.int32, (8, 128), 0)
    lane = lanes_of((8, 128))
    cell = lax.broadcasted_iota(jnp.int32, (128, 128), 0)
    slab = jnp.zeros((8, 128), jnp.float32)
    last = jnp.zeros((8, 128), jnp.float32)
    for u in (0, 1):
        weight = jnp.where(slot < count_ref[u], precision_ref[u : u + 1, :], 0.0)
        both = jnp.where(sub == 0, weight, jnp.where(sub == 1, weight * value_ref[u : u + 1, :], 0.0))
        site = site_ref[u : u + 1, :]
        in_slab = ((cell & 63) == site) & ((cell >> 6) == u)
        in_last = ((64 + (cell & 15)) == site) & (((cell >> 4) & 1) == u)
        dims = (((1,), (1,)), ((), ()))
        slab += lax.dot_general(
            both, in_slab.astype(jnp.float32), dims, precision=HIGHEST,
            preferred_element_type=jnp.float32,
        )
        last += lax.dot_general(
            both, in_last.astype(jnp.float32), dims, precision=HIGHEST,
            preferred_element_type=jnp.float32,
        )
    out = jnp.where(sub < 2, slab, jnp.where(sub < 4, pltpu.roll(last, 2, 0), 0.0))
    for t in (0, 1):
        gain = []
        for u in (0, 1):
            total = jnp.float32(0.0)
            for n in range(3):
                total += jnp.where(near_ref[t, n] == u, loc_ref[t, n], 0.0)
            gain.append(total)
        out = jnp.where(sub == 4 + t, jnp.where((lane >> 6) == 0, gain[0], gain[1]), out)
        out = jnp.where(sub == 6 + t, jnp.where(((lane >> 4) & 1) == 0, gain[0], gain[1]), out)
    out_ref[...] = out


def split(x):
    head = x.astype(jnp.bfloat16)
    return head, (x - head.astype(jnp.float32)).astype(jnp.bfloat16)


def product(left, right, axis):
    return lax.dot_general(
        jnp.concatenate([left[0], left[1], left[0]], axis=1),
        jnp.concatenate([right[0], right[0], right[1]], axis=axis),
        (((1,), (axis,)), ((), ())),
        preferred_element_type=jnp.float32,
    )


def analysis_kernel(half_ref, own_ref, other_ref, own_stats_ref, other_stats_ref, out_ref):
    lane8 = lanes_of((8, 128))
    sub8 = lax.broadcasted_iota(jnp.int32, (8, 128), 0)
    lane = lanes_of((MEMBERS, 128))
    lane1 = lanes_of((1, 128))
    slabs = []
    for b in (0, 1):
        slabs.append(
            jnp.concatenate(
                [
                    ref[s * 20 + 8 * b : s * 20 + 8 * b + 8, :]
                    for ref in (own_ref, other_ref)
                    for s in range(8)
                ],
                axis=0,
            )
        )
    parts = []
    for ref in (own_ref, other_ref):
        for s in range(8):
            four = ref[s * 20 + 16 : s * 20 + 20, :]
            eight = jnp.concatenate([four, four], axis=0)
            eight = jnp.where(sub8 < 4, eight, pltpu.roll(eight, 64, 1))
            parts.append(jnp.where(lane8 < 64, eight, 0.0))
    slabs.append(jnp.concatenate(parts, axis=0))
    means = [jnp.sum(x, axis=0, keepdims=True) * (1.0 / MEMBERS) for x in slabs]
    slabs = [x - m for x, m in zip(slabs, means)]
    first = half_ref[0] == 0
    own = own_stats_ref[...]
    other = other_stats_ref[...]
    stats = [jnp.where(first, own, other), jnp.where(first, other, own)]
    eye = (lax.broadcasted_iota(jnp.int32, (MEMBERS, 128), 0) == lane).astype(jnp.float32)
    tiles = [(b, t) for b in (0, 1) for t in (0, 1)]
    tops, fields, norms = [], [], []
    for b, t in tiles:
        s = stats[b]
        mine = (lane1 >> 5) == b
        gain = s[4 + t : 5 + t]
        gain_last = jnp.where(mine, s[6 + t : 7 + t], 0.0)
        pull = gain * (s[1:2] - s[0:1] * means[b])
        pull_last = gain_last * (s[3:4] - s[2:3] * means[2])
        p, r = slabs[b], slabs[2]
        gram = product(
            split(jnp.concatenate([p * (gain * s[0:1]), r * (gain_last * s[2:3])], axis=1)),
            split(jnp.concatenate([p, r], axis=1)),
            1,
        )
        gram = gram + (MEMBERS - 1.0) * eye
        norm = jnp.sqrt(jnp.sum(jnp.sum(gram * gram, axis=0, keepdims=True), axis=1, keepdims=True))
        norms.append(norm)
        tops.append(gram * (1.0 / norm))
        b_col = jnp.sum(p * pull + r * pull_last, axis=1, keepdims=True)
        if t == 0:
            field = jnp.where(
                lane < 64, p, jnp.where((lane >> 4) == 4 + 2 * b, pltpu.roll(r, 64, 1), 0.0)
            )
            field = jnp.where(lane == 127, b_col, field)
        else:
            field = jnp.where(lane >= 64, p, jnp.where((lane >> 4) == 2 * b + 1, r, 0.0))
            field = jnp.where(lane == 0, b_col, field)
        fields.append(field)
    for sweep in range(NSI):
        factors = [split(1.5 * eye - 0.5 * x) for x in tops]
        if sweep < NSI - 1:
            both = [
                product(f, split(jnp.concatenate([x, y], axis=1)), 0)
                for f, x, y in zip(factors, tops, fields)
            ]
            fields = [x[:, 128:] for x in both]
            tops = [product(split(x[:, :128]), f, 0) for f, x in zip(factors, both)]
        else:
            fields = [product(f, split(y), 0) for f, y in zip(factors, fields)]
    moved = []
    for (b, t), field, norm in zip(tiles, fields, norms):
        column = field[:, 127:128] if t == 0 else field[:, 0:1]
        shift = jnp.sum(column * field, axis=0, keepdims=True) * (1.0 / norm)
        moved.append(field[:64] * jnp.sqrt((MEMBERS - 1.0) / norm) + shift)
    lane64 = lanes_of((64, 128))
    outs = [
        jnp.where(lane64 < 64, moved[0], moved[1]) + means[0],
        jnp.where(lane64 < 64, moved[2], moved[3]) + means[1],
    ]
    group = lane64 >> 4
    last = jnp.where(group == 1, moved[1], pltpu.roll(moved[0], 64, 1))
    last = jnp.where(group == 2, pltpu.roll(moved[2], 64, 1), last)
    last = jnp.where(group == 3, moved[3], last) + means[2]
    for d in range(8):
        for b in (0, 1):
            out_ref[d * 20 + 8 * b : d * 20 + 8 * b + 8, :] = outs[b][8 * d : 8 * d + 8]
        piece = last[8 * d : 8 * d + 8]
        out_ref[d * 20 + 16 : d * 20 + 20, :] = jnp.where(
            lane8[:4] < 64, piece[:4], pltpu.roll(piece, 64, 1)[4:]
        )


def unpack_kernel(band_ref, in_ref, near_ref, far_ref):
    lane = lanes_of((8, 128))
    sub = lax.broadcasted_iota(jnp.int32, (8, 128), 0)
    group = lane >> 4
    lasts = []
    for q in range(8):
        four = in_ref[q * 20 + 16 : q * 20 + 20, :]
        eight = jnp.concatenate([four, four], axis=0)
        lasts.append(jnp.where(sub < 4, eight, pltpu.roll(eight, 64, 1)))
    def field(r, v):
        b, result = r // 2, None
        for j in range(4):
            q = (r % 2) * 4 + j
            if v < 4:
                slab = in_ref[q * 20 + 8 * b : q * 20 + 8 * b + 8, :]
                for u in (0, 1):
                    piece = turned(slab, 2 * j + u - 4 * u - v)
                    result = piece if result is None else jnp.where(group == 2 * j + u, piece, result)
            else:
                piece = turned(lasts[q], 2 * j - 2 * b)
                result = piece if result is None else jnp.where((group >> 1) == j, piece, result)
        return result

    for v in range(5):
        for r in (0, 1):
            at = (v * 2 + r) * 8
            far, near = ordered(band_ref, field(2 + r, v), field(r, v))
            near_ref[at : at + 8, :] = near
            far_ref[at : at + 8, :] = far


def forecast_kernel(band_ref, near_ref, far_ref, from_near_ref, from_far_ref, out_ref):
    below, low, high, above = [], [], [], []
    for r in (0, 1):
        at = [slice((v * 2 + r) * 8, (v * 2 + r) * 8 + 8) for v in range(5)]
        own = [ordered(band_ref, near_ref[x, :], far_ref[x, :]) for x in at]
        got = [ordered(band_ref, from_near_ref[x, :], from_far_ref[x, :]) for x in at]
        low.append([x for x, _ in own])
        high.append([x for _, x in own])
        below.append([x for x, _ in got])
        above.append([x for _, x in got])
    rows = below + low + high + above
    rows = transport(rows)
    for r in range(4):
        for v in range(5):
            out_ref[pl.ds(v * 4 + r, 8, stride=20), :] = rows[r][v]


def array(*shape):
    return jax.ShapeDtypeStruct(shape, jnp.float32)


def call(kernel, in_specs, *out):
    return pl.pallas_call(
        kernel,
        out_shape=out if len(out) > 1 else out[0],
        in_specs=in_specs,
        out_specs=(VMEM,) * len(out) if len(out) > 1 else VMEM,
        compiler_params=SMALL,
    )


def swap(x, axis, first):
    pairs = [(i, i + 1) for i in range(first, lax.axis_size(axis) - 1, 2)]
    return lax.ppermute(x, axis, pairs + [(b, a) for a, b in pairs])


def exchange(x):
    return lax.all_to_all(
        x.reshape(8, 5, 4, 128), "q", split_axis=0, concat_axis=0, tiled=True
    ).reshape(160, 128)


def shards(ensemble, obs_value, obs_site, obs_count, obs_precision, loc_weight, neighbours):
    band = jnp.reshape(lax.axis_index("band"), (1,))
    half = jnp.reshape(lax.axis_index("half"), (1,))
    fields = ensemble.transpose(1, 2, 0, 3).reshape(160, 128)
    near = swap(fields, "band", 0)
    far = swap(fields, "band", 1)
    stats = call(statistics_kernel, [SMEM] * 3 + [VMEM] * 3, array(8, 128))(
        obs_count, loc_weight, neighbours, obs_value, obs_site, obs_precision
    )
    packed, payload = call(
        functools.partial(background_kernel, lax.axis_size("band")),
        [SMEM] + [VMEM] * 4, array(160, 128), array(168, 128),
    )(band, fields, near, far, stats)
    payload = swap(payload, "half", 0)
    own = exchange(packed)
    other, other_stats = call(
        strip_kernel, [VMEM, VMEM, SMEM], array(160, 128), array(8, 128)
    )(payload, own, half)
    other = exchange(other)
    analysed = call(analysis_kernel, [SMEM] + [VMEM] * 4, array(160, 128))(
        half, own, other, stats, other_stats
    )
    near, far = call(
        unpack_kernel, [SMEM, VMEM], array(80, 128), array(80, 128)
    )(band, exchange(analysed))
    from_near = swap(near, "band", 0)
    from_far = swap(far, "band", 1)
    out = call(forecast_kernel, [SMEM] + [VMEM] * 4, array(160, 128))(
        band, near, far, from_near, from_far
    )
    return out.reshape(8, 5, 4, 128)


def solution(mesh):
    bands = mesh.shape["band"]
    fine = Mesh(mesh.devices.reshape(bands, 2, 8), ("band", "half", "q"))
    members = ("half", "q")
    tiles = ("band", "half", "q")
    return jax.shard_map(
        shards,
        mesh=fine,
        in_specs=(
            P(members, None, "band", None),
            P(tiles, None),
            P(tiles, None),
            P(tiles),
            P(tiles, None),
            P(tiles, None),
            P(tiles, None),
        ),
        out_specs=P(members, None, "band", None),
        check_vma=False,
    )
```

```python
import functools

import jax
import jax.numpy as jnp
from jax import lax
from jax.experimental import pallas as pl
from jax.experimental.pallas import tpu as pltpu
from jax.sharding import Mesh, PartitionSpec as P

NSI = 6
COURANT = 0.08
HIGHEST = lax.Precision.HIGHEST
MEMBERS = 128
VMEM = pl.BlockSpec(memory_space=pltpu.VMEM)
SMEM = pl.BlockSpec(memory_space=pltpu.SMEM)
SMALL = pltpu.CompilerParams(vmem_limit_bytes=8 * 2**20)


def half_minmod(lower, upper):
    return 0.5 * (
        jnp.maximum(0.0, jnp.minimum(lower, upper)) + jnp.minimum(0.0, jnp.maximum(lower, upper))
    )


def twice_flux(left, right, carrier):
    speed = jnp.maximum(jnp.abs(left[carrier]), jnp.abs(right[carrier]))
    gain_left = left[carrier] + speed
    gain_right = right[carrier] - speed
    return [gain_left * l + gain_right * r for l, r in zip(left, right)]


def transport(rows):
    count, variables = len(rows), range(len(rows[0]))
    jumps = [[rows[i + 1][v] - rows[i][v] for v in variables] for i in range(count - 1)]
    halves = [None] + [
        [half_minmod(jumps[i - 1][v], jumps[i][v]) for v in variables] for i in range(1, count - 1)
    ]
    fluxes = [None] + [
        twice_flux(
            [rows[i][v] + halves[i][v] for v in variables],
            [rows[i + 1][v] - halves[i + 1][v] for v in variables],
            1,
        )
        for i in range(1, count - 2)
    ]
    result = []
    for i in range(2, count - 2):
        left, right = [], []
        for v in variables:
            q = rows[i][v]
            jump = pltpu.roll(q, 127, 1) - q
            half = half_minmod(pltpu.roll(jump, 1, 1), jump)
            left.append(q + half)
            right.append(pltpu.roll(q - half, 127, 1))
        flux = twice_flux(left, right, 0)
        result.append(
            [
                rows[i][v]
                - (0.5 * COURANT)
                * ((fluxes[i][v] - fluxes[i - 1][v]) + (flux[v] - pltpu.roll(flux[v], 1, 1)))
                for v in variables
            ]
        )
    return result


def turned(x, groups):
    shift = (16 * groups) % 128
    return pltpu.roll(x, shift, 1) if shift else x


def lanes_of(shape):
    return lax.broadcasted_iota(jnp.int32, shape, 1)


def ordered(band_ref, near, far):
    even = jnp.full(near.shape, (band_ref[0] & 1) == 0)
    return jnp.where(even, far, near), jnp.where(even, near, far)


def background_kernel(bands, band_ref, centre_ref, near_ref, far_ref, stats_ref, out_ref):
    out_ref[160:168, :] = stats_ref[...]
    low, centre, high = [], [], []
    for r in range(4):
        at = [slice((v * 4 + r) * 8, (v * 4 + r) * 8 + 8) for v in range(5)]
        pairs = [ordered(band_ref, near_ref[x, :], far_ref[x, :]) for x in at]
        low.append([below for below, _ in pairs])
        centre.append([centre_ref[x, :] for x in at])
        high.append([above for _, above in pairs])
    rows = low + centre + high
    rows = transport(rows)
    keep_low = (band_ref[0] > 0).astype(jnp.float32)
    keep_high = (band_ref[0] < bands - 1).astype(jnp.float32)
    for i in (0, 1):
        rows[i] = [x * keep_low for x in rows[i]]
    for i in (6, 7):
        rows[i] = [x * keep_high for x in rows[i]]
    rows = transport(rows)
    lane = lanes_of((8, 128))
    group = lane >> 4
    for q in range(8):
        j = q % 4
        chosen = (q // 4, 2 + q // 4)
        for b in (0, 1):
            slab = None
            for g in range(8):
                u, v = g // 4, g % 4
                piece = turned(rows[chosen[b]][v], g - (2 * j + u))
                slab = piece if slab is None else jnp.where(group == g, piece, slab)
            out_ref[q * 20 + 8 * b : q * 20 + 8 * b + 8, :] = slab
        last = jnp.where(
            lane < 32, turned(rows[chosen[0]][4], -2 * j), turned(rows[chosen[1]][4], 2 - 2 * j)
        )
        out_ref[q * 20 + 16 : q * 20 + 20, :] = jnp.where(
            lane[:4] < 64, last[:4], pltpu.roll(last, 64, 1)[4:]
        )


def fields_kernel(in_ref, out_ref):
    out_ref[...] = in_ref[:160, :]


def strip_kernel(in_ref, own_ref, half_ref, out_ref, stats_ref):
    out_ref[...] = in_ref[:160, :]
    stats_ref[...] = in_ref[160:168, :]


def statistics_kernel(count_ref, loc_ref, near_ref, value_ref, site_ref, precision_ref, out_ref):
    slot = lanes_of((1, 128))
    sub = lax.broadcasted_iota(jnp.int32, (8, 128), 0)
    lane = lanes_of((8, 128))
    cell = lax.broadcasted_iota(jnp.int32, (128, 128), 0)
    slab = jnp.zeros((8, 128), jnp.float32)
    last = jnp.zeros((8, 128), jnp.float32)
    for u in (0, 1):
        weight = jnp.where(slot < count_ref[u], precision_ref[u : u + 1, :], 0.0)
        both = jnp.where(sub == 0, weight, jnp.where(sub == 1, weight * value_ref[u : u + 1, :], 0.0))
        site = site_ref[u : u + 1, :]
        in_slab = ((cell & 63) == site) & ((cell >> 6) == u)
        in_last = ((64 + (cell & 15)) == site) & (((cell >> 4) & 1) == u)
        dims = (((1,), (1,)), ((), ()))
        slab += lax.dot_general(
            both, in_slab.astype(jnp.float32), dims, precision=HIGHEST,
            preferred_element_type=jnp.float32,
        )
        last += lax.dot_general(
            both, in_last.astype(jnp.float32), dims, precision=HIGHEST,
            preferred_element_type=jnp.float32,
        )
    out = jnp.where(sub < 2, slab, jnp.where(sub < 4, pltpu.roll(last, 2, 0), 0.0))
    for t in (0, 1):
        gain = []
        for u in (0, 1):
            total = jnp.float32(0.0)
            for n in range(3):
                total += jnp.where(near_ref[t, n] == u, loc_ref[t, n], 0.0)
            gain.append(total)
        out = jnp.where(sub == 4 + t, jnp.where((lane >> 6) == 0, gain[0], gain[1]), out)
        out = jnp.where(sub == 6 + t, jnp.where(((lane >> 4) & 1) == 0, gain[0], gain[1]), out)
    out_ref[...] = out


def split(x):
    head = x.astype(jnp.bfloat16)
    return head, (x - head.astype(jnp.float32)).astype(jnp.bfloat16)


def product(left, right, axis):
    return lax.dot_general(
        jnp.concatenate([left[0], left[1], left[0]], axis=1),
        jnp.concatenate([right[0], right[0], right[1]], axis=axis),
        (((1,), (axis,)), ((), ())),
        preferred_element_type=jnp.float32,
    )


def analysis_kernel(half_ref, own_ref, other_ref, own_stats_ref, other_stats_ref, out_ref):
    lane8 = lanes_of((8, 128))
    sub8 = lax.broadcasted_iota(jnp.int32, (8, 128), 0)
    lane = lanes_of((MEMBERS, 128))
    lane1 = lanes_of((1, 128))
    slabs = []
    for b in (0, 1):
        slabs.append(
            jnp.concatenate(
                [
                    ref[s * 20 + 8 * b : s * 20 + 8 * b + 8, :]
                    for ref in (own_ref, other_ref)
                    for s in range(8)
                ],
                axis=0,
            )
        )
    parts = []
    for ref in (own_ref, other_ref):
        for s in range(8):
            four = ref[s * 20 + 16 : s * 20 + 20, :]
            eight = jnp.concatenate([four, four], axis=0)
            eight = jnp.where(sub8 < 4, eight, pltpu.roll(eight, 64, 1))
            parts.append(jnp.where(lane8 < 64, eight, 0.0))
    slabs.append(jnp.concatenate(parts, axis=0))
    means = [jnp.sum(x, axis=0, keepdims=True) * (1.0 / MEMBERS) for x in slabs]
    slabs = [x - m for x, m in zip(slabs, means)]
    first = half_ref[0] == 0
    own = own_stats_ref[...]
    other = other_stats_ref[...]
    stats = [jnp.where(first, own, other), jnp.where(first, other, own)]
    eye = (lax.broadcasted_iota(jnp.int32, (MEMBERS, 128), 0) == lane).astype(jnp.float32)
    tiles = [(b, t) for b in (0, 1) for t in (0, 1)]
    tops, fields, norms = [], [], []
    for b, t in tiles:
        s = stats[b]
        mine = (lane1 >> 5) == b
        gain = s[4 + t : 5 + t]
        gain_last = jnp.where(mine, s[6 + t : 7 + t], 0.0)
        pull = gain * (s[1:2] - s[0:1] * means[b])
        pull_last = gain_last * (s[3:4] - s[2:3] * means[2])
        p, r = slabs[b], slabs[2]
        gram = product(
            split(jnp.concatenate([p * (gain * s[0:1]), r * (gain_last * s[2:3])], axis=1)),
            split(jnp.concatenate([p, r], axis=1)),
            1,
        )
        gram = gram + (MEMBERS - 1.0) * eye
        norm = jnp.sqrt(jnp.sum(jnp.sum(gram * gram, axis=0, keepdims=True), axis=1, keepdims=True))
        norms.append(norm)
        tops.append(gram * (1.0 / norm))
        b_col = jnp.sum(p * pull + r * pull_last, axis=1, keepdims=True)
        if t == 0:
            field = jnp.where(
                lane < 64, p, jnp.where((lane >> 4) == 4 + 2 * b, pltpu.roll(r, 64, 1), 0.0)
            )
            field = jnp.where(lane == 127, b_col, field)
        else:
            field = jnp.where(lane >= 64, p, jnp.where((lane >> 4) == 2 * b + 1, r, 0.0))
            field = jnp.where(lane == 0, b_col, field)
        fields.append(field)
    for sweep in range(NSI):
        factors = [split(1.5 * eye - 0.5 * x) for x in tops]
        if sweep < NSI - 1:
            both = [
                product(f, split(jnp.concatenate([x, y], axis=1)), 0)
                for f, x, y in zip(factors, tops, fields)
            ]
            fields = [x[:, 128:] for x in both]
            tops = [product(split(x[:, :128]), f, 0) for f, x in zip(factors, both)]
        else:
            fields = [product(f, split(y), 0) for f, y in zip(factors, fields)]
    moved = []
    for (b, t), field, norm in zip(tiles, fields, norms):
        column = field[:, 127:128] if t == 0 else field[:, 0:1]
        shift = jnp.sum(column * field, axis=0, keepdims=True) * (1.0 / norm)
        moved.append(field[:64] * jnp.sqrt((MEMBERS - 1.0) / norm) + shift)
    lane64 = lanes_of((64, 128))
    outs = [
        jnp.where(lane64 < 64, moved[0], moved[1]) + means[0],
        jnp.where(lane64 < 64, moved[2], moved[3]) + means[1],
    ]
    group = lane64 >> 4
    last = jnp.where(group == 1, moved[1], pltpu.roll(moved[0], 64, 1))
    last = jnp.where(group == 2, pltpu.roll(moved[2], 64, 1), last)
    last = jnp.where(group == 3, moved[3], last) + means[2]
    for d in range(8):
        for b in (0, 1):
            out_ref[d * 20 + 8 * b : d * 20 + 8 * b + 8, :] = outs[b][8 * d : 8 * d + 8]
        piece = last[8 * d : 8 * d + 8]
        out_ref[d * 20 + 16 : d * 20 + 20, :] = jnp.where(
            lane8[:4] < 64, piece[:4], pltpu.roll(piece, 64, 1)[4:]
        )


def unpack_kernel(band_ref, in_ref, near_ref, far_ref):
    lane = lanes_of((8, 128))
    sub = lax.broadcasted_iota(jnp.int32, (8, 128), 0)
    group = lane >> 4
    lasts = []
    for q in range(8):
        four = in_ref[q * 20 + 16 : q * 20 + 20, :]
        eight = jnp.concatenate([four, four], axis=0)
        lasts.append(jnp.where(sub < 4, eight, pltpu.roll(eight, 64, 1)))
    def field(r, v):
        b, result = r // 2, None
        for j in range(4):
            q = (r % 2) * 4 + j
            if v < 4:
                slab = in_ref[q * 20 + 8 * b : q * 20 + 8 * b + 8, :]
                for u in (0, 1):
                    piece = turned(slab, 2 * j + u - 4 * u - v)
                    result = piece if result is None else jnp.where(group == 2 * j + u, piece, result)
            else:
                piece = turned(lasts[q], 2 * j - 2 * b)
                result = piece if result is None else jnp.where((group >> 1) == j, piece, result)
        return result

    for v in range(5):
        for r in (0, 1):
            at = (v * 2 + r) * 8
            far, near = ordered(band_ref, field(2 + r, v), field(r, v))
            near_ref[at : at + 8, :] = near
            far_ref[at : at + 8, :] = far


def forecast_kernel(band_ref, near_ref, far_ref, from_near_ref, from_far_ref, out_ref):
    below, low, high, above = [], [], [], []
    for r in (0, 1):
        at = [slice((v * 2 + r) * 8, (v * 2 + r) * 8 + 8) for v in range(5)]
        own = [ordered(band_ref, near_ref[x, :], far_ref[x, :]) for x in at]
        got = [ordered(band_ref, from_near_ref[x, :], from_far_ref[x, :]) for x in at]
        low.append([x for x, _ in own])
        high.append([x for _, x in own])
        below.append([x for x, _ in got])
        above.append([x for _, x in got])
    rows = below + low + high + above
    rows = transport(rows)
    for r in range(4):
        for v in range(5):
            out_ref[pl.ds(v * 4 + r, 8, stride=20), :] = rows[r][v]


def array(*shape):
    return jax.ShapeDtypeStruct(shape, jnp.float32)


def call(kernel, in_specs, *out):
    return pl.pallas_call(
        kernel,
        out_shape=out if len(out) > 1 else out[0],
        in_specs=in_specs,
        out_specs=(VMEM,) * len(out) if len(out) > 1 else VMEM,
        compiler_params=SMALL,
    )


def swap(x, axis, first):
    pairs = [(i, i + 1) for i in range(first, lax.axis_size(axis) - 1, 2)]
    return lax.ppermute(x, axis, pairs + [(b, a) for a, b in pairs])


def exchange(x):
    return lax.all_to_all(
        x.reshape(8, 5, 4, 128), "q", split_axis=0, concat_axis=0, tiled=True
    ).reshape(160, 128)


def shards(ensemble, obs_value, obs_site, obs_count, obs_precision, loc_weight, neighbours):
    band = jnp.reshape(lax.axis_index("band"), (1,))
    half = jnp.reshape(lax.axis_index("half"), (1,))
    fields = ensemble.transpose(1, 2, 0, 3).reshape(160, 128)
    near = swap(fields, "band", 0)
    far = swap(fields, "band", 1)
    stats = call(statistics_kernel, [SMEM] * 3 + [VMEM] * 3, array(8, 128))(
        obs_count, loc_weight, neighbours, obs_value, obs_site, obs_precision
    )
    mine = call(
        functools.partial(background_kernel, lax.axis_size("band")),
        [SMEM] + [VMEM] * 4, array(168, 128),
    )(band, fields, near, far, stats)
    payload = swap(mine, "half", 0)
    packed = call(fields_kernel, [VMEM], array(160, 128))(mine)
    own = exchange(packed)
    other, other_stats = call(
        strip_kernel, [VMEM, VMEM, SMEM], array(160, 128), array(8, 128)
    )(payload, own, half)
    other = exchange(other)
    analysed = call(analysis_kernel, [SMEM] + [VMEM] * 4, array(160, 128))(
        half, own, other, stats, other_stats
    )
    near, far = call(
        unpack_kernel, [SMEM, VMEM], array(80, 128), array(80, 128)
    )(band, exchange(analysed))
    from_near = swap(near, "band", 0)
    from_far = swap(far, "band", 1)
    out = call(forecast_kernel, [SMEM] + [VMEM] * 4, array(160, 128))(
        band, near, far, from_near, from_far
    )
    return out.reshape(8, 5, 4, 128)


def solution(mesh):
    bands = mesh.shape["band"]
    fine = Mesh(mesh.devices.reshape(bands, 2, 8), ("band", "half", "q"))
    members = ("half", "q")
    tiles = ("band", "half", "q")
    return jax.shard_map(
        shards,
        mesh=fine,
        in_specs=(
            P(members, None, "band", None),
            P(tiles, None),
            P(tiles, None),
            P(tiles),
            P(tiles, None),
            P(tiles, None),
            P(tiles, None),
        ),
        out_specs=P(members, None, "band", None),
        check_vma=False,
    )
```
